128 devices in a mesh: wide: 16 (over z, x_hi, core), narrow: 8 (over y, x_lo).
Axes of the slice: x: 4 (x_hi: 2, x_lo: 2; x = x_hi * 2 + x_lo), y: 4, z: 4, core: 2. Of those that a mesh axis runs over, the one named last changes fastest.
Arguments:
- homolog_embedding: float32 [64, 1024, 256], P('wide', 'narrow'), may hold values from -6 to 6
- pair_state: float32 [1024, 1024, 128], P('wide', 'narrow'), may hold values from -6 to 6
- probe_projector: float32 [256, 256], replicated, may hold values from -0.375 to 0.375
- lookup_projector: float32 [256, 256], replicated, may hold values from -0.375 to 0.375
- content_projector: float32 [256, 256], replicated, may hold values from -0.375 to 0.375
- sigmoid_projector: float32 [256, 256], replicated, may hold values from -0.375 to 0.375
- sigmoid_offset: float32 [256], replicated, may hold values from -4 to 4
- pair_bias_weight: float32 [128, 8], replicated, may hold values from -4 to 4
- mixing_projector: float32 [256, 256], replicated, may hold values from -0.375 to 0.375
- mixing_offset: float32 [256], replicated, may hold values from -3 to 3
- first_factor_projector: float32 [256, 32], replicated, may hold values from -0.375 to 0.375
- second_factor_projector: float32 [256, 32], replicated, may hold values from -0.375 to 0.375
- outer_product_weight: float32 [1024, 128], replicated, may hold values from -0.5 to 0.5
- outer_product_bias: float32 [128], replicated, may hold values from -3 to 3
- up_weight: float32 [128, 512], replicated, may hold values from -0.5 to 0.5
- expand_bias: float32 [512], replicated, may hold values from -3 to 3
- down_weight: float32 [512, 128], replicated, may hold values from -0.25 to 0.25
Outputs:
- alignment_state_next: float32 [64, 1024, 256], P('wide', 'narrow')
- pair_state_next: float32 [1024, 1024, 128], P('wide', 'narrow')
The draws below stay inside these ranges and needn't reach their ends.
All inputs are finite; a program needn't handle non-finite values.
Results may differ from the reference program's by a relative error of at most 0.0003.
Values sent between devices are 32-bit elements; how exact they have to be, the bound alone decides.
A program may use at most 128 MiB of HBM per device.

```python
import math
import jax
import jax.numpy as jnp
from jax import lax

FEATURE_DEPTH = 256
CZ = 128
H = 8
HIDDEN_FACTORS = 32
AMINO_SPAN = 1024
HEAD_SIZE = 32
FT = 512
ALIGNED_CHAINS = 64


def draw_pair_state(key, part):
    normal_part = jax.random.normal(key, (AMINO_SPAN, AMINO_SPAN, CZ), jnp.float32)
    return jnp.clip(normal_part, -6.0, 6.0)


def draw_pair_bias_weight(key, part):
    weights = jnp.clip(jax.random.normal(key, (CZ, H), jnp.float32) * CZ ** (-0.5), -0.6, 0.6)
    return weights


def block_levels(own_key, extent, split, least, high):
    factor_of = 1.0
    for dim, parts in split:
        steps = jax.random.uniform(jax.random.fold_in(jax.random.fold_in(own_key, 6), dim), (parts,), jnp.float32, least / len(split), high / len(split))
        factor_of = factor_of * jnp.repeat(jnp.exp(steps), extent[dim] // parts).reshape((-1,) + (1,) * (len(extent) - 1 - dim))
    return factor_of


def centred(key, shape, width, bound, split=(), kind=jnp.bfloat16):
    array = width * jax.random.normal(key, shape, jnp.float32)
    if split:
        array = array * block_levels(key, shape, split, -0.22, 0.18)
    return jnp.clip(array, -bound, bound).astype(kind)


def setup_inputs(seed: int = 0) -> dict:
    splits = jax.random.split(jax.random.key(seed), 18)
    return {
        "homolog_embedding": centred(splits[0], (ALIGNED_CHAINS, AMINO_SPAN, FEATURE_DEPTH), 1.0, 6.0, ((0, 16), (1, 8)), jnp.float32),
        "pair_state": draw_pair_state(jax.random.fold_in(splits[17], 71), 0),
        "probe_projector": centred(splits[2], (FEATURE_DEPTH, FEATURE_DEPTH), FEATURE_DEPTH ** -0.5, 0.375, (), jnp.float32),
        "lookup_projector": centred(splits[3], (FEATURE_DEPTH, FEATURE_DEPTH), FEATURE_DEPTH ** -0.5, 0.375, (), jnp.float32),
        "content_projector": centred(splits[4], (FEATURE_DEPTH, FEATURE_DEPTH), FEATURE_DEPTH ** -0.5, 0.375, (), jnp.float32),
        "sigmoid_projector": centred(splits[5], (FEATURE_DEPTH, FEATURE_DEPTH), FEATURE_DEPTH ** -0.5, 0.375, (), jnp.float32),
        "sigmoid_offset": centred(splits[6], (FEATURE_DEPTH,), 1.0, 4.0, (), jnp.float32),
        "pair_bias_weight": draw_pair_bias_weight(jax.random.fold_in(splits[17], 71), 0),
        "mixing_projector": centred(splits[8], (FEATURE_DEPTH, FEATURE_DEPTH), FEATURE_DEPTH ** -0.5, 0.375, (), jnp.float32),
        "mixing_offset": centred(splits[9], (FEATURE_DEPTH,), 0.5, 3.0, (), jnp.float32),
        "first_factor_projector": centred(splits[10], (FEATURE_DEPTH, HIDDEN_FACTORS), FEATURE_DEPTH ** -0.5, 0.375, (), jnp.float32),
        "second_factor_projector": centred(splits[11], (FEATURE_DEPTH, HIDDEN_FACTORS), FEATURE_DEPTH ** -0.5, 0.375, (), jnp.float32),
        "outer_product_weight": centred(splits[12], (HIDDEN_FACTORS * HIDDEN_FACTORS, CZ), (HIDDEN_FACTORS * HIDDEN_FACTORS // 8) ** -0.5, 0.5, (), jnp.float32),
        "outer_product_bias": centred(splits[13], (CZ,), 0.5, 3.0, (), jnp.float32),
        "up_weight": centred(splits[14], (CZ, FT), CZ ** -0.5, 0.5, (), jnp.float32),
        "expand_bias": centred(splits[15], (FT,), 0.5, 3.0, (), jnp.float32),
        "down_weight": centred(splits[16], (FT, CZ), FT ** -0.5, 0.25, (), jnp.float32),
    }


finest_precision = lax.Precision.HIGHEST

def layer_normalize(tensor):
    row_mean = lax.optimization_barrier(jnp.mean(tensor, axis=-1, keepdims=True))
    centered = tensor - row_mean
    variance = lax.optimization_barrier(jnp.mean(centered * centered, axis=-1, keepdims=True))
    return centered * lax.rsqrt(variance + 1e-05)

def matrix_multiply(first_arr, second_arr):
    return jnp.dot(first_arr, second_arr, precision=finest_precision, preferred_element_type=jnp.float32)

def reference(homolog_embedding, pair_state, probe_projector, lookup_projector, content_projector, sigmoid_projector, sigmoid_offset, pair_bias_weight, mixing_projector, mixing_offset, first_factor_projector, second_factor_projector, outer_product_weight, outer_product_bias, up_weight, expand_bias, down_weight):
    alignment_normed = layer_normalize(homolog_embedding)
    query_vectors = matrix_multiply(alignment_normed, probe_projector) / math.sqrt(HEAD_SIZE)
    key_rows = matrix_multiply(alignment_normed, lookup_projector)
    value_rows = matrix_multiply(alignment_normed, content_projector)
    gate_logits = matrix_multiply(alignment_normed, sigmoid_projector) + sigmoid_offset
    pair_bias = jnp.einsum('ijc,ch->hij', layer_normalize(pair_state), pair_bias_weight, precision=finest_precision)

    def per_sequence(operands):
        query_seq = operands[0].reshape(AMINO_SPAN, H, HEAD_SIZE)
        key_seq = operands[1].reshape(AMINO_SPAN, H, HEAD_SIZE)
        content_by_homolog = operands[2].reshape(AMINO_SPAN, H, HEAD_SIZE)
        scores = jnp.einsum('ihd,jhd->hij', query_seq, key_seq, precision=finest_precision) + pair_bias
        row_max = lax.optimization_barrier(jnp.max(scores, axis=-1, keepdims=True))
        exponent = jnp.exp(scores - row_max)
        softmax_probabilities = exponent / lax.optimization_barrier(jnp.sum(exponent, axis=-1, keepdims=True))
        returned_tensor = jnp.einsum('arz,zas->ras', softmax_probabilities, content_by_homolog, precision=finest_precision).reshape(AMINO_SPAN, FEATURE_DEPTH)
        return returned_tensor * jax.nn.sigmoid(operands[3])
    attended_values = lax.map(per_sequence, (query_vectors, key_rows, value_rows, gate_logits))
    alignment_state_next = homolog_embedding + matrix_multiply(attended_values, mixing_projector) + mixing_offset
    outer_product_normed = layer_normalize(alignment_state_next)
    left_proj = matrix_multiply(outer_product_normed, first_factor_projector)
    right_proj = matrix_multiply(outer_product_normed, second_factor_projector)
    row_block = min(32, AMINO_SPAN)

    def outer_rows(block_index):
        left_part = lax.dynamic_slice_in_dim(left_proj, block_index * row_block, row_block, 1)
        product = jnp.einsum('sic,sjd->ijcd', left_part, right_proj, precision=finest_precision) / ALIGNED_CHAINS
        flat = product.reshape(row_block * AMINO_SPAN, HIDDEN_FACTORS * HIDDEN_FACTORS)
        return matrix_multiply(flat, outer_product_weight).reshape(row_block, AMINO_SPAN, CZ)
    update = lax.map(outer_rows, jnp.arange(AMINO_SPAN // row_block, dtype=jnp.int32)).reshape(AMINO_SPAN, AMINO_SPAN, CZ)
    pair_mid = pair_state + update + outer_product_bias

    def transition(pair_rows):
        hidden = jax.nn.relu(matrix_multiply(layer_normalize(pair_rows), up_weight) + expand_bias)
        return pair_rows + matrix_multiply(hidden, down_weight)
    pair_state_next = lax.map(transition, pair_mid.reshape(AMINO_SPAN // row_block, row_block, AMINO_SPAN, CZ)).reshape(AMINO_SPAN, AMINO_SPAN, CZ)
    return (alignment_state_next, pair_state_next)
```

```python
import functools
import math

import jax
import jax.numpy as jnp
from jax import lax
from jax.experimental import pallas as pl
from jax.experimental.pallas import tpu as pltpu
from jax.sharding import PartitionSpec as P

F32 = jnp.float32
BF16 = jnp.bfloat16
LOG2E = math.log2(math.e)
VMEM_LIMIT = 60 * 1024 * 1024
MESH = pl.DeviceIdType.MESH

NT = (((1,), (1,)), ((), ()))


def dot(a, b):
    return jnp.dot(a, b, preferred_element_type=F32)


def split(x):
    hi = x.astype(BF16)
    lo = (x - hi.astype(F32)).astype(BF16)
    return hi, lo


def split32(x):
    hi = x.astype(BF16).astype(F32)
    return hi, (x - hi).astype(BF16).astype(F32)


def dot3(a_hi, a_lo, b_hi, b_lo):
    return dot(a_hi, b_hi) + dot(a_hi, b_lo) + dot(a_lo, b_hi)


def normalize(x):
    mean = jnp.mean(x, axis=-1, keepdims=True)
    centered = x - mean
    variance = jnp.mean(centered * centered, axis=-1, keepdims=True)
    return centered * lax.rsqrt(variance + 1e-5)


def whole(memory_space=pltpu.VMEM):
    return pl.BlockSpec(memory_space=memory_space)


def full(shape):
    return pl.BlockSpec(shape, lambda *_: (0,) * len(shape))


def bias_kernel(pair_ref, weight_ref, out_ref):
    rows, cols, channels = pair_ref.shape
    heads = weight_ref.shape[0]
    normed = normalize(pair_ref[...].reshape(rows * cols, channels))
    n_hi, n_lo = split(normed)
    stacked = jnp.concatenate([n_hi, n_lo], axis=1)
    w_hi, w_lo = split32(weight_ref[...] * LOG2E)
    top = jnp.concatenate([w_hi, w_hi], axis=1)
    low = jnp.concatenate([w_lo, jnp.zeros_like(w_lo)], axis=1)
    weights = jnp.concatenate([top, low], axis=0).astype(BF16)
    both = lax.dot_general(weights, stacked, NT, preferred_element_type=F32)
    result = both[:heads] + both[heads:]
    for row in range(rows):
        out_ref[:, row, :] = result[:, row * cols : (row + 1) * cols]


def pair_bias(pair_state, weight_t):
    rows, cols, channels = pair_state.shape
    heads = weight_t.shape[0]
    step = 8
    return pl.pallas_call(
        bias_kernel,
        grid=(rows // step,),
        in_specs=[
            pl.BlockSpec((step, cols, channels), lambda i: (i, 0, 0)),
            full((heads, channels)),
        ],
        out_specs=pl.BlockSpec((heads, step, cols), lambda i: (0, i, 0)),
        out_shape=jax.ShapeDtypeStruct((heads, rows, cols), F32),
        compiler_params=pltpu.CompilerParams(vmem_limit_bytes=VMEM_LIMIT),
        name="pair_bias",
    )(pair_state, weight_t)


def project_kernel(x_ref, q_ref, k_ref, v_ref, g_ref, off_ref, out_ref, gate_ref):
    seqs, res, channels = x_ref.shape
    heads = out_ref.shape[0]
    width = channels // heads
    per_tile = 128 // width
    normed = normalize(x_ref[...].reshape(seqs * res, channels))
    n_hi, n_lo = split(normed)
    scale = LOG2E / math.sqrt(width)
    for kind, ref in enumerate((q_ref, k_ref, v_ref)):
        w_hi, w_lo = split(ref[...])
        y = dot3(n_hi, n_lo, w_hi, w_lo)
        if kind == 0:
            y = y * scale
        for s in range(seqs):
            for tile in range(channels // 128):
                part = y[s * res : (s + 1) * res, tile * 128 : (tile + 1) * 128].T
                for h in range(per_tile):
                    out_ref[tile * per_tile + h, s, kind * width : (kind + 1) * width, :] = part[
                        h * width : (h + 1) * width
                    ]
    w_hi, w_lo = split(g_ref[...])
    gate = jax.nn.sigmoid(dot3(n_hi, n_lo, w_hi, w_lo) + off_ref[...])
    gate_ref[...] = gate.reshape(seqs, res, channels)


def project(x, wq, wk, wv, wg, offset, heads):
    seqs, res, channels = x.shape
    width = channels // heads
    return pl.pallas_call(
        project_kernel,
        in_specs=[whole()] * 6,
        out_specs=[whole(), whole()],
        out_shape=[
            jax.ShapeDtypeStruct((heads, seqs, 3 * width, res), F32),
            jax.ShapeDtypeStruct((seqs, res, channels), F32),
        ],
        compiler_params=pltpu.CompilerParams(vmem_limit_bytes=VMEM_LIMIT),
        name="project",
    )(x, wq, wk, wv, wg, offset.reshape(1, channels))


def place(wide, narrow):
    return {"wide": wide, "narrow": narrow}


def greet(peers):
    barrier = pltpu.get_barrier_semaphore()
    for peer in peers:
        pl.semaphore_signal(barrier, inc=1, device_id=peer, device_id_type=MESH)
    pl.semaphore_wait(barrier, len(peers))


def remote(src, dst, send, recv, peer):
    return pltpu.make_async_remote_copy(
        src_ref=src, dst_ref=dst, send_sem=send, recv_sem=recv, device_id=peer, device_id_type=MESH
    )


def wide_links(wide):
    z, x, core = wide // 4, (wide // 2) % 2, wide % 2
    at = lambda z_, x_, c_: (z_ * 2 + x_) * 2 + c_
    up, down, far = (z + 1) % 4, (z + 3) % 4, (z + 2) % 4
    return z, x, core, at, up, down, far


def gather_wide(buf, rows, send, recv):
    wide, narrow = lax.axis_index("wide"), lax.axis_index("narrow")
    z, x, core, at, up, down, far = wide_links(wide)
    other_x, other_core = 1 - x, 1 - core
    half = rows // 2

    def slab(z_, x_, c_, part=None):
        start = at(z_, x_, c_) * rows
        if part is None:
            return buf.at[pl.ds(start, rows)]
        return buf.at[pl.ds(start + part * half, half)]

    up_dev = place(at(up, x, core), narrow)
    down_dev = place(at(down, x, core), narrow)
    x_dev = place(at(z, other_x, core), narrow)
    core_dev = place(at(z, x, other_core), narrow)
    started = []
    count = [0]

    def push(region, index, dev):
        copy = remote(region, region, send.at[index], recv.at[index], dev)
        copy.start()
        started.append(copy)

    def arrived(region, index):
        remote(region, region, send.at[index], recv.at[index], core_dev).wait_recv()

    own = slab(z, x, core)
    push(own, 1, up_dev)
    push(own, 2, down_dev)
    push(own, 0, x_dev)
    push(own, 9, core_dev)
    expected = [(slab(z, x, other_core), 9)]

    def side(s, x_):
        below, above = slab(down, x_, core), slab(up, x_, core)
        base = 1 + 4 * s
        arrived(below, base)
        push(slab(down, x_, core, 0), base + 2, up_dev)
        push(below, 9 + base, core_dev)
        arrived(above, base + 1)
        push(slab(up, x_, core, 1), base + 3, down_dev)
        push(above, 9 + base + 1, core_dev)

    def finish(s, x_):
        base = 1 + 4 * s
        for part in range(2):
            region = slab(far, x_, core, part)
            arrived(region, base + 2 + part)
            push(region, 9 + base + 2 + part, core_dev)

    def partner(s, x_):
        base = 9 + 1 + 4 * s
        expected.append((slab(down, x_, other_core), base))
        expected.append((slab(up, x_, other_core), base + 1))
        for part in range(2):
            expected.append((slab(far, x_, other_core, part), base + 2 + part))

    cross = slab(z, other_x, core)
    arrived(cross, 0)
    push(cross, 5, up_dev)
    push(cross, 6, down_dev)
    push(cross, 18, core_dev)
    expected.append((slab(z, other_x, other_core), 18))
    side(0, x)
    finish(0, x)
    side(1, other_x)
    finish(1, other_x)
    partner(0, x)
    partner(1, other_x)
    for region, index in expected:
        arrived(region, index)
    for copy in started:
        copy.wait_send()


def wide_peers():
    wide, narrow = lax.axis_index("wide"), lax.axis_index("narrow")
    z, x, core, at, up, down, far = wide_links(wide)
    return [
        place(at(up, x, core), narrow),
        place(at(down, x, core), narrow),
        place(at(z, 1 - x, core), narrow),
        place(at(z, x, 1 - core), narrow),
    ]


def narrow_peers():
    wide, narrow = lax.axis_index("wide"), lax.axis_index("narrow")
    return [place(wide, narrow ^ k) for k in range(1, 8)]


def heads_kernel(qkv, bias, qkv_out, bias_out, local, b_send, b_recv, q_send, q_recv, send, recv):
    wide, narrow = lax.axis_index("wide"), lax.axis_index("narrow")
    rows, cols = bias.shape[1:]
    greet(narrow_peers() + wide_peers())

    def bias_slot(source):
        return bias_out.at[pl.ds(wide * rows, rows), pl.ds(source * cols, cols)]

    own_bias = pltpu.make_async_copy(bias.at[narrow], bias_slot(narrow), local.at[0])
    own_bias.start()
    copies = []
    for k in range(1, 8):
        peer = narrow ^ k
        copy = remote(
            bias.at[peer], bias_slot(narrow), b_send.at[k], b_recv.at[k], place(wide, peer)
        )
        copy.start()
        copies.append(copy)
    own_qkv = pltpu.make_async_copy(qkv.at[narrow], qkv_out.at[narrow], local.at[1])
    own_qkv.start()
    for k in range(1, 8):
        peer = narrow ^ k
        copy = remote(
            qkv.at[peer], qkv_out.at[narrow], q_send.at[k], q_recv.at[k], place(wide, peer)
        )
        copy.start()
        copies.append(copy)
    own_bias.wait()
    for k in range(1, 8):
        slot = bias_slot(narrow ^ k)
        remote(slot, slot, b_send.at[k], b_recv.at[k], place(wide, narrow ^ k)).wait_recv()
    gather_wide(bias_out, rows, send, recv)
    for k in range(1, 8):
        slot = qkv_out.at[narrow ^ k]
        remote(slot, slot, q_send.at[k], q_recv.at[k], place(wide, narrow ^ k)).wait_recv()
    own_qkv.wait()
    for copy in copies:
        copy.wait_send()


DMA = pltpu.SemaphoreType.DMA


def exchange_heads(qkv, bias, wide_size):
    heads, rows, cols = bias.shape
    return pl.pallas_call(
        heads_kernel,
        in_specs=[whole(), whole()],
        out_specs=[whole(pl.ANY), whole(pl.ANY)],
        out_shape=[
            jax.ShapeDtypeStruct(qkv.shape, F32),
            jax.ShapeDtypeStruct((wide_size * rows, heads * cols), F32),
        ],
        scratch_shapes=[DMA((2,)), DMA((8,)), DMA((8,)), DMA((8,)), DMA((8,)), DMA((19,)), DMA((19,))],
        compiler_params=pltpu.CompilerParams(
            collective_id=0, has_side_effects=True, vmem_limit_bytes=VMEM_LIMIT
        ),
        name="exchange_heads",
    )(qkv, bias)


def swap_kernel(src, out, local, send, recv):
    wide, narrow = lax.axis_index("wide"), lax.axis_index("narrow")
    greet(narrow_peers())
    copies = []
    for k in range(1, 8):
        peer = narrow ^ k
        copy = remote(src.at[peer], out.at[narrow], send.at[k], recv.at[k], place(wide, peer))
        copy.start()
        copies.append(copy)
    own = pltpu.make_async_copy(src.at[narrow], out.at[narrow], local)
    own.start()
    for k in range(1, 8):
        slot = out.at[narrow ^ k]
        remote(slot, slot, send.at[k], recv.at[k], place(wide, narrow ^ k)).wait_recv()
    own.wait()
    for copy in copies:
        copy.wait_send()


def exchange_back(src):
    return pl.pallas_call(
        swap_kernel,
        in_specs=[whole()],
        out_specs=whole(pl.ANY),
        out_shape=jax.ShapeDtypeStruct(src.shape, F32),
        scratch_shapes=[DMA, DMA((8,)), DMA((8,))],
        compiler_params=pltpu.CompilerParams(
            collective_id=1, has_side_effects=True, vmem_limit_bytes=VMEM_LIMIT
        ),
        name="exchange_back",
    )(src)


def factors_kernel(left, right, left_out, right_out, local, l_send, l_recv, send, recv):
    wide, narrow = lax.axis_index("wide"), lax.axis_index("narrow")
    seqs = right.shape[0]
    barrier = pltpu.get_barrier_semaphore()
    source_narrow = wide // 2
    for w in range(16):
        me = jnp.logical_and(wide == w, narrow == source_narrow)

        @pl.when(jnp.logical_not(me))
        def _():
            pl.semaphore_signal(
                barrier, inc=1, device_id=place(w, source_narrow), device_id_type=MESH
            )

    for peer in wide_peers():
        pl.semaphore_signal(barrier, inc=1, device_id=peer, device_id_type=MESH)
    selfish = (wide // 2) == narrow
    pl.semaphore_wait(barrier, 2 * 8 - selfish.astype(jnp.int32) + 4)

    own_right = pltpu.make_async_copy(right, right_out.at[pl.ds(wide * seqs, seqs)], local.at[0])
    own_right.start()

    def target(half, k):
        return 2 * narrow + half, narrow ^ k

    def left_copy(half, k):
        w, n = target(half, k)
        return remote(
            left.at[half], left_out.at[wide], l_send.at[half, k], l_recv.at[wide], place(w, n)
        )

    own_left = pltpu.make_async_copy(left.at[wide % 2], left_out.at[wide], local.at[1])
    for k in range(8):
        for half in range(2):
            me = jnp.logical_and(selfish, wide % 2 == half) if k == 0 else None
            if me is None:
                left_copy(half, k).start()
            else:

                @pl.when(jnp.logical_not(me))
                def _():
                    left_copy(half, k).start()

                @pl.when(me)
                def _():
                    own_left.start()

    own_right.wait()
    gather_wide(right_out, seqs, send, recv)

    for w in range(16):
        me = jnp.logical_and(selfish, wide == w)

        @pl.when(jnp.logical_not(me))
        def _():
            slot = left_out.at[w]
            remote(
                slot, slot, l_send.at[0, 0], l_recv.at[w], place(w, source_narrow)
            ).wait_recv()

    @pl.when(selfish)
    def _():
        own_left.wait()

    for k in range(8):
        for half in range(2):
            if k:
                left_copy(half, k).wait_send()
            else:
                me = jnp.logical_and(selfish, wide % 2 == half)

                @pl.when(jnp.logical_not(me))
                def _():
                    left_copy(half, k).wait_send()


def exchange_factors(left, right, wide_size):
    return pl.pallas_call(
        factors_kernel,
        in_specs=[whole(), whole()],
        out_specs=[whole(pl.ANY), whole(pl.ANY)],
        out_shape=[
            jax.ShapeDtypeStruct((wide_size, *left.shape[1:]), F32),
            jax.ShapeDtypeStruct((wide_size * right.shape[0], *right.shape[1:]), F32),
        ],
        scratch_shapes=[DMA((2,)), DMA((2, 8)), DMA((16,)), DMA((19,)), DMA((19,))],
        compiler_params=pltpu.CompilerParams(
            collective_id=2, has_side_effects=True, vmem_limit_bytes=VMEM_LIMIT
        ),
        name="exchange_factors",
    )(left, right)


def attention_kernel(qkv_ref, bias_ref, out_ref, q_s, k_s, v_s, w_s):
    blocks, seqs, stacked, res = qkv_ref.shape
    width = stacked // 3

    @pl.when(pl.program_id(0) == 0)
    def _():
        pad = jnp.zeros((width, res), F32)
        for s in range(seqs):
            for b in range(blocks):
                cols = slice(b * res, (b + 1) * res)
                q_hi, q_lo = split32(qkv_ref[b, s, 0:width, :])
                k_hi, k_lo = split32(qkv_ref[b, s, width : 2 * width, :])
                v_hi, v_lo = split32(qkv_ref[b, s, 2 * width :, :])
                q_s[s, cols, :] = jnp.concatenate([q_hi, q_hi, q_lo, q_lo], axis=0).T.astype(BF16)
                k_s[s, :, cols] = jnp.concatenate([k_hi, k_lo, k_hi, k_lo], axis=0).astype(BF16)
                one = jnp.ones_like(pad)
                v_s[s, cols, :] = jnp.concatenate([v_hi, v_lo, one, pad], axis=0).T.astype(BF16)
                w_s[s, cols, :] = jnp.concatenate([v_hi, pad, one, pad], axis=0).T.astype(BF16)

    block = pl.program_id(0)
    bias = bias_ref[...]
    start = pl.multiple_of(block * res, res)
    for s in range(seqs):
        scores = dot(q_s[s, pl.ds(start, res), :], k_s[s]) + bias
        top = jnp.max(scores, axis=-1, keepdims=True)
        weights = jnp.exp2(scores - top)
        p_hi, p_lo = split(weights)
        mixed = (dot(p_hi, v_s[s]) + dot(p_lo, w_s[s])).T
        out_ref[0, s] = (mixed[:width] + mixed[width : 2 * width]) / mixed[2 * width : 3 * width]


def attention(qkv, bias):
    blocks, seqs, stacked, res = qkv.shape
    width = stacked // 3
    span = blocks * res
    return pl.pallas_call(
        attention_kernel,
        grid=(blocks,),
        in_specs=[full(qkv.shape), pl.BlockSpec((res, span), lambda i: (i, 0))],
        out_specs=pl.BlockSpec((1, seqs, width, res), lambda i: (i, 0, 0, 0)),
        out_shape=jax.ShapeDtypeStruct((blocks, seqs, width, res), F32),
        scratch_shapes=[
            pltpu.VMEM((seqs, span, 4 * width), BF16),
            pltpu.VMEM((seqs, 4 * width, span), BF16),
            pltpu.VMEM((seqs, span, 4 * width), BF16),
            pltpu.VMEM((seqs, span, 4 * width), BF16),
        ],
        compiler_params=pltpu.CompilerParams(vmem_limit_bytes=VMEM_LIMIT),
        name="attention",
    )(qkv, bias)


def mix_kernel(o_ref, gate_ref, x_ref, w_ref, off_ref, f_ref, s_ref, next_ref, left_ref, right_ref):
    heads, seqs, width, res = o_ref.shape
    channels = heads * width
    w_hi, w_lo = split(w_ref[...])
    pieces = []
    for s in range(seqs):
        stacked = o_ref[:, s].reshape(channels, res)
        pieces.append(stacked.T)
    attended = jnp.concatenate(pieces, axis=0) * gate_ref[...].reshape(seqs * res, channels)
    a_hi, a_lo = split(attended)
    x = x_ref[...].reshape(seqs * res, channels)
    after = x + dot3(a_hi, a_lo, w_hi, w_lo) + off_ref[...]
    next_ref[...] = after.reshape(seqs, res, channels)
    n_hi, n_lo = split(normalize(after))
    first = f_ref[...]
    factors = jnp.concatenate([first] * 4 + [s_ref[...]] * 4, axis=1)
    f_hi, f_lo = split(factors)
    y = dot3(n_hi, n_lo, f_hi, f_lo)
    hidden = first.shape[1]
    quarter = lax.broadcasted_iota(jnp.int32, (res // 8, 128), 1) // hidden
    for s in range(seqs):
        left = y[s * res : (s + 1) * res, :128]
        for half in range(2):
            rows = left[half * res // 2 : (half + 1) * res // 2].reshape(4, res // 8, 128)
            picked = rows[0]
            for q in range(1, 4):
                picked = jnp.where(quarter == q, rows[q], picked)
            left_ref[half, s] = picked
        right_ref[s] = y[s * res : (s + 1) * res, 128:].T[:hidden]


def mix(o, gate, x, w, offset, first, second):
    seqs, res, channels = x.shape
    hidden = first.shape[1]
    return pl.pallas_call(
        mix_kernel,
        in_specs=[whole()] * 7,
        out_specs=[whole()] * 3,
        out_shape=[
            jax.ShapeDtypeStruct(x.shape, F32),
            jax.ShapeDtypeStruct((2, seqs, res // 8, 128), F32),
            jax.ShapeDtypeStruct((seqs, hidden, res), F32),
        ],
        compiler_params=pltpu.CompilerParams(vmem_limit_bytes=VMEM_LIMIT),
        name="mix",
    )(o, gate, x, w, offset.reshape(1, channels), first, second)


def pair_kernel(
    left_ref, right_ref, pair_ref, w_ref, ob_ref, up_ref, eb_ref, down_ref, out_ref,
    l_s, r_s, wt_s, u_s, d_s, oh_s, ol_s,
):
    seqs, groups, _ = left_ref.shape
    hidden, cols = right_ref.shape[1:]
    channels = pair_ref.shape[-1]
    span = hidden * hidden

    @pl.when(pl.program_id(0) == 0)
    def _():
        for r in range(groups):
            hi, lo = split32(left_ref[:, r, :])
            l_s[r * 128 : (r + 1) * 128, 0:128] = jnp.concatenate([hi, hi], axis=0).T.astype(BF16)
            l_s[r * 128 : (r + 1) * 128, 128:256] = jnp.concatenate([lo, lo], axis=0).T.astype(BF16)
        for d in range(hidden):
            hi, lo = split(right_ref[:, d, :])
            part = slice(d * cols, (d + 1) * cols)
            r_s[:, part] = jnp.concatenate([hi, lo, hi, lo], axis=0)
        for b in range(span // 128):
            rows = [w_ref[pl.ds(b * 4 + e, hidden, stride=hidden), :] for e in range(4)]
            w_hi, w_lo = split32(jnp.concatenate(rows, axis=0).T)
            wt_s[0:channels, b * 128 : (b + 1) * 128] = w_hi.astype(BF16)
            wt_s[channels : 2 * channels, b * 128 : (b + 1) * 128] = w_lo.astype(BF16)
        u_hi, u_lo = split(up_ref[...])
        u_s[0:channels] = u_hi
        u_s[channels : 2 * channels] = u_hi
        u_s[2 * channels :] = u_lo
        d_hi, d_lo = split(down_ref[...])
        d_s[:, 0:channels] = d_hi
        d_s[:, channels:] = d_lo

    step = pl.program_id(0)
    lhs = l_s[pl.ds(pl.multiple_of(step * 256, 256), 256), :]
    for d2 in range(hidden // 2):
        o_hi, o_lo = split(dot(lhs, r_s[:, d2 * 2 * cols : (d2 + 1) * 2 * cols]))
        for r2 in range(2):
            for q in range(4):
                rows = slice((r2 * 4 + q) * hidden, (r2 * 4 + q + 1) * hidden)
                for e in range(2):
                    d = d2 * 2 + e
                    at = (q, slice(d * hidden, (d + 1) * hidden), slice(r2 * cols, (r2 + 1) * cols))
                    oh_s[at] = o_hi[rows, e * cols : (e + 1) * cols]
                    ol_s[at] = o_lo[rows, e * cols : (e + 1) * cols]
    for q in range(4):
        first = dot(wt_s[...], oh_s[q])
        update = first[:channels] + first[channels:] + dot(wt_s[0:channels], ol_s[q])
        update = update.T * (1.0 / seqs)
        mid = pair_ref[q].reshape(2 * cols, channels) + update + ob_ref[...]
        n_hi, n_lo = split(normalize(mid))
        pre = dot(jnp.concatenate([n_hi, n_lo], axis=1), u_s[0 : 2 * channels])
        pre = pre + dot(n_hi, u_s[2 * channels :])
        h_hi, h_lo = split(jnp.maximum(pre + eb_ref[...], 0.0))
        wide = dot(h_hi, d_s[...])
        result = mid + wide[:, :channels] + wide[:, channels:] + dot(h_lo, d_s[:, 0:channels])
        out_ref[q] = result.reshape(2, cols, channels)


def pair_update(left, right, pair_state, w, ob, up, eb, down):
    rows, cols, channels = pair_state.shape
    seqs, groups, lanes = left.shape
    hidden = right.shape[1]
    ft = up.shape[1]
    view = pair_state.reshape(4, rows // 4, cols, channels)
    block = pl.BlockSpec((4, 2, cols, channels), lambda i: (0, i, 0, 0))
    out = pl.pallas_call(
        pair_kernel,
        grid=(rows // 8,),
        in_specs=[
            full(left.shape),
            full(right.shape),
            block,
            full(w.shape),
            full((1, channels)),
            full(up.shape),
            full((1, ft)),
            full(down.shape),
        ],
        out_specs=block,
        out_shape=jax.ShapeDtypeStruct(view.shape, F32),
        scratch_shapes=[
            pltpu.VMEM((groups * lanes, 4 * seqs), BF16),
            pltpu.VMEM((4 * seqs, hidden * cols), BF16),
            pltpu.VMEM((2 * channels, hidden * hidden), BF16),
            pltpu.VMEM((3 * channels, ft), BF16),
            pltpu.VMEM((ft, 2 * channels), BF16),
            pltpu.VMEM((4, hidden * hidden, 2 * cols), BF16),
            pltpu.VMEM((4, hidden * hidden, 2 * cols), BF16),
        ],
        compiler_params=pltpu.CompilerParams(vmem_limit_bytes=VMEM_LIMIT),
        name="pair_update",
    )(left, right, view, w, ob.reshape(1, channels), up, eb.reshape(1, ft), down)
    return out.reshape(pair_state.shape)


def per_device(
    homolog_embedding,
    pair_state,
    probe_projector,
    lookup_projector,
    content_projector,
    sigmoid_projector,
    sigmoid_offset,
    pair_bias_weight,
    mixing_projector,
    mixing_offset,
    first_factor_projector,
    second_factor_projector,
    outer_product_weight,
    outer_product_bias,
    up_weight,
    expand_bias,
    down_weight,
):
    heads = pair_bias_weight.shape[1]
    wide_size = lax.axis_size("wide")
    bias = pair_bias(pair_state, pair_bias_weight.T)
    qkv, gate = project(
        homolog_embedding,
        probe_projector,
        lookup_projector,
        content_projector,
        sigmoid_projector,
        sigmoid_offset,
        heads,
    )
    qkv_all, bias_all = exchange_heads(qkv, bias, wide_size)
    mixed = attention(qkv_all, bias_all)
    back = exchange_back(mixed)
    after, left, right = mix(
        back,
        gate,
        homolog_embedding,
        mixing_projector,
        mixing_offset,
        first_factor_projector,
        second_factor_projector,
    )
    left_all, right_all = exchange_factors(left, right, wide_size)
    left_all = left_all.reshape(-1, *left_all.shape[2:])
    pair_next = pair_update(
        left_all,
        right_all,
        pair_state,
        outer_product_weight,
        outer_product_bias,
        up_weight,
        expand_bias,
        down_weight,
    )
    return after, pair_next


def solution(mesh):
    split_spec = P("wide", "narrow", None)
    return jax.shard_map(
        per_device,
        mesh=mesh,
        in_specs=(split_spec, split_spec) + (P(),) * 15,
        out_specs=(split_spec, split_spec),
        check_vma=False,
    )
```

```python
import functools
import math

import jax
import jax.numpy as jnp
from jax import lax
from jax.experimental import pallas as pl
from jax.experimental.pallas import tpu as pltpu
from jax.sharding import PartitionSpec as P

F32 = jnp.float32
BF16 = jnp.bfloat16
LOG2E = math.log2(math.e)
MIB = 1024 * 1024
MESH = pl.DeviceIdType.MESH

NT = (((1,), (1,)), ((), ()))


def dot(a, b):
    return jnp.dot(a, b, preferred_element_type=F32)


def dot_nt(a, b):
    return lax.dot_general(a, b, NT, preferred_element_type=F32)


def split(x):
    hi = x.astype(BF16)
    lo = (x - hi.astype(F32)).astype(BF16)
    return hi, lo


def split32(x):
    hi = x.astype(BF16).astype(F32)
    return hi, (x - hi).astype(BF16).astype(F32)


def dot3(a_hi, a_lo, b_hi, b_lo):
    return dot(a_hi, b_hi) + dot(a_hi, b_lo) + dot(a_lo, b_hi)


def normalize(x):
    mean = jnp.mean(x, axis=-1, keepdims=True)
    centered = x - mean
    variance = jnp.mean(centered * centered, axis=-1, keepdims=True)
    return centered * lax.rsqrt(variance + 1e-5)


def whole(memory_space=pltpu.VMEM):
    return pl.BlockSpec(memory_space=memory_space)


def full(shape):
    return pl.BlockSpec(shape, lambda *_: (0,) * len(shape))


def bias_rows(pair, w_t):
    rows, cols, channels = pair.shape
    heads = w_t.shape[0]
    n_hi, n_lo = split(normalize(pair.reshape(rows * cols, channels)))
    w_hi, w_lo = split32(w_t * LOG2E)
    top = jnp.concatenate([w_hi, w_hi], axis=1)
    low = jnp.concatenate([w_lo, jnp.zeros_like(w_lo)], axis=1)
    weights = jnp.concatenate([top, low], axis=0).astype(BF16)
    both = dot_nt(weights, jnp.concatenate([n_hi, n_lo], axis=1))
    return both[:heads] + both[heads:]


def place(wide, narrow):
    return {"wide": wide, "narrow": narrow}


def greet(peers):
    barrier = pltpu.get_barrier_semaphore()
    for peer in peers:
        pl.semaphore_signal(barrier, inc=1, device_id=peer, device_id_type=MESH)
    pl.semaphore_wait(barrier, len(peers))


def remote(src, dst, send, recv, peer):
    return pltpu.make_async_remote_copy(
        src_ref=src, dst_ref=dst, send_sem=send, recv_sem=recv, device_id=peer, device_id_type=MESH
    )


def wide_links(wide):
    z, x, core = wide // 4, (wide // 2) % 2, wide % 2
    at = lambda z_, x_, c_: (z_ * 2 + x_) * 2 + c_
    up, down, far = (z + 1) % 4, (z + 3) % 4, (z + 2) % 4
    return z, x, core, at, up, down, far


def gather_wide(buf, rows, send, recv, source=None, then=None):
    wide, narrow = lax.axis_index("wide"), lax.axis_index("narrow")
    z, x, core, at, up, down, far = wide_links(wide)
    other_x, other_core = 1 - x, 1 - core
    half = rows // 2

    def slab(z_, x_, c_, part=None):
        start = at(z_, x_, c_) * rows
        if part is None:
            return buf.at[pl.ds(start, rows)]
        return buf.at[pl.ds(start + part * half, half)]

    up_dev = place(at(up, x, core), narrow)
    down_dev = place(at(down, x, core), narrow)
    x_dev = place(at(z, other_x, core), narrow)
    core_dev = place(at(z, x, other_core), narrow)
    started = []
    count = [0]

    def push(region, index, dev):
        copy = remote(region, region, send.at[index], recv.at[index], dev)
        copy.start()
        started.append(copy)

    def arrived(region, index):
        remote(region, region, send.at[index], recv.at[index], core_dev).wait_recv()

    own = slab(z, x, core)
    for index, dev in ((0, x_dev), (1, up_dev), (2, down_dev), (9, core_dev)):
        copy = remote(own if source is None else source, own, send.at[index], recv.at[index], dev)
        copy.start()
        started.append(copy)
    if then is not None:
        then()
    expected = [(slab(z, x, other_core), 9)]

    def side(s, x_):
        below, above = slab(down, x_, core), slab(up, x_, core)
        base = 1 + 4 * s
        arrived(below, base)
        push(slab(down, x_, core, 0), base + 2, up_dev)
        push(below, 9 + base, core_dev)
        arrived(above, base + 1)
        push(slab(up, x_, core, 1), base + 3, down_dev)
        push(above, 9 + base + 1, core_dev)

    def finish(s, x_):
        base = 1 + 4 * s
        for part in range(2):
            region = slab(far, x_, core, part)
            arrived(region, base + 2 + part)
            push(region, 9 + base + 2 + part, core_dev)

    def partner(s, x_):
        base = 9 + 1 + 4 * s
        expected.append((slab(down, x_, other_core), base))
        expected.append((slab(up, x_, other_core), base + 1))
        for part in range(2):
            expected.append((slab(far, x_, other_core, part), base + 2 + part))

    cross = slab(z, other_x, core)
    arrived(cross, 0)
    push(cross, 5, up_dev)
    push(cross, 6, down_dev)
    push(cross, 18, core_dev)
    expected.append((slab(z, other_x, other_core), 18))
    side(0, x)
    finish(0, x)
    side(1, other_x)
    finish(1, other_x)
    partner(0, x)
    partner(1, other_x)
    for region, index in expected:
        arrived(region, index)
    for copy in started:
        copy.wait_send()


def wide_peers():
    wide, narrow = lax.axis_index("wide"), lax.axis_index("narrow")
    z, x, core, at, up, down, far = wide_links(wide)
    return [
        place(at(up, x, core), narrow),
        place(at(down, x, core), narrow),
        place(at(z, 1 - x, core), narrow),
        place(at(z, x, 1 - core), narrow),
    ]


def narrow_peers():
    wide, narrow = lax.axis_index("wide"), lax.axis_index("narrow")
    return [place(wide, narrow ^ k) for k in range(1, 8)]


BIAS_STEP = 32


def heads_kernel(
    x, wq, wk, wv, wg, offset, pair, weight, qkv_out, bias_out, gate_out,
    x_s, w_s, wb_s, tile, qkv, bias,
    load, load_w, local, b_send, b_recv, q_send, q_recv, send, recv,
):
    wide, narrow = lax.axis_index("wide"), lax.axis_index("narrow")
    rows, cols = bias.shape[1:]
    seqs, res, channels = x.shape
    heads = qkv.shape[0]
    width = channels // heads
    per_tile = 128 // width
    parts = rows // BIAS_STEP
    first_loads = [pltpu.make_async_copy(x, x_s, load_w.at[4])]
    for index, w in enumerate((wq, wk, wv, wg)):
        first_loads.append(pltpu.make_async_copy(w, w_s.at[index], load_w.at[index]))
    first_loads.append(pltpu.make_async_copy(weight, wb_s, load_w.at[5]))
    for copy in first_loads:
        copy.start()
    loads = []
    for part in range(parts):
        span = pl.ds(part * BIAS_STEP, BIAS_STEP)
        copy = pltpu.make_async_copy(pair.at[span], tile.at[span], load.at[part])
        copy.start()
        loads.append(copy)
    for copy in first_loads:
        copy.wait()

    n_hi, n_lo = split(normalize(x_s[...].reshape(seqs * res, channels)))
    scale = LOG2E / math.sqrt(width)
    for kind in range(3):
        y = dot3(n_hi, n_lo, *split(w_s[kind]))
        if kind == 0:
            y = y * scale
        for s in range(seqs):
            for t in range(channels // 128):
                turned = y[s * res : (s + 1) * res, t * 128 : (t + 1) * 128].T
                for h in range(per_tile):
                    qkv[t * per_tile + h, s, kind * width : (kind + 1) * width, :] = turned[
                        h * width : (h + 1) * width
                    ]
    greet(narrow_peers() + wide_peers())
    copies = []

    def send_qkv(ks):
        for k in ks:
            peer = narrow ^ k
            copy = remote(
                qkv.at[peer], qkv_out.at[narrow], q_send.at[k], q_recv.at[k], place(wide, peer)
            )
            copy.start()
            copies.append(copy)

    send_qkv((1, 2, 6))
    own_qkv = pltpu.make_async_copy(qkv.at[narrow], qkv_out.at[narrow], local.at[1])
    own_qkv.start()
    for part in range(parts):
        loads[part].wait()
        first = part * BIAS_STEP
        result = bias_rows(tile[first : first + BIAS_STEP], wb_s[...])
        for row in range(BIAS_STEP):
            bias[:, first + row, :] = result[:, row * cols : (row + 1) * cols]

    def bias_slot(source):
        return bias_out.at[pl.ds(wide * rows, rows), pl.ds(source * cols, cols)]

    own_bias = pltpu.make_async_copy(bias.at[narrow], bias_slot(narrow), local.at[0])
    own_bias.start()
    for k in (1, 3, 7, 5, 2, 6, 4):
        peer = narrow ^ k
        copy = remote(
            bias.at[peer], bias_slot(narrow), b_send.at[k], b_recv.at[k], place(wide, peer)
        )
        copy.start()
        copies.append(copy)
    own_bias.wait()
    for k in range(1, 8):
        slot = bias_slot(narrow ^ k)
        remote(slot, slot, b_send.at[k], b_recv.at[k], place(wide, narrow ^ k)).wait_recv()

    def rest():
        send_qkv((3, 7, 5, 4))
        gate = dot3(n_hi, n_lo, *split(w_s[3])) + offset[...]
        gate_out[...] = jax.nn.sigmoid(gate).reshape(seqs, res, channels)

    gather_wide(bias_out, rows, send, recv, then=rest)
    for k in range(1, 8):
        slot = qkv_out.at[narrow ^ k]
        remote(slot, slot, q_send.at[k], q_recv.at[k], place(wide, narrow ^ k)).wait_recv()
    own_qkv.wait()
    for copy in copies:
        copy.wait_send()


DMA = pltpu.SemaphoreType.DMA


def exchange_heads(x, wq, wk, wv, wg, offset, pair_state, weight_t, wide_size):
    rows, cols, _ = pair_state.shape
    heads, pair_channels = weight_t.shape
    seqs, res, channels = x.shape
    width = channels // heads
    qkv = (heads, seqs, 3 * width, res)
    return pl.pallas_call(
        heads_kernel,
        in_specs=[whole(pltpu.HBM)] * 5 + [whole(), whole(pltpu.HBM), whole(pltpu.HBM)],
        out_specs=[whole(pl.ANY), whole(pl.ANY), whole()],
        out_shape=[
            jax.ShapeDtypeStruct(qkv, F32),
            jax.ShapeDtypeStruct((wide_size * rows, heads * cols), F32),
            jax.ShapeDtypeStruct(x.shape, F32),
        ],
        scratch_shapes=[
            pltpu.VMEM(x.shape, F32),
            pltpu.VMEM((4, channels, channels), F32),
            pltpu.VMEM((heads, pair_channels), F32),
            pltpu.VMEM(pair_state.shape, F32),
            pltpu.VMEM(qkv, F32),
            pltpu.VMEM((heads, rows, cols), F32),
            DMA((rows // BIAS_STEP,)),
            DMA((6,)),
            DMA((2,)),
            DMA((8,)),
            DMA((8,)),
            DMA((8,)),
            DMA((8,)),
            DMA((19,)),
            DMA((19,)),
        ],
        compiler_params=pltpu.CompilerParams(
            collective_id=0, has_side_effects=True, vmem_limit_bytes=54 * MIB
        ),
        name="exchange_heads",
    )(x, wq, wk, wv, wg, offset.reshape(1, channels), pair_state, weight_t)


def swap_kernel(src, out, local, send, recv):
    wide, narrow = lax.axis_index("wide"), lax.axis_index("narrow")
    greet(narrow_peers())
    copies = []
    for k in range(1, 8):
        peer = narrow ^ k
        copy = remote(src.at[peer], out.at[narrow], send.at[k], recv.at[k], place(wide, peer))
        copy.start()
        copies.append(copy)
    own = pltpu.make_async_copy(src.at[narrow], out.at[narrow], local)
    own.start()
    for k in range(1, 8):
        slot = out.at[narrow ^ k]
        remote(slot, slot, send.at[k], recv.at[k], place(wide, narrow ^ k)).wait_recv()
    own.wait()
    for copy in copies:
        copy.wait_send()


def exchange_back(src):
    return pl.pallas_call(
        swap_kernel,
        in_specs=[whole()],
        out_specs=whole(pl.ANY),
        out_shape=jax.ShapeDtypeStruct(src.shape, F32),
        scratch_shapes=[DMA, DMA((8,)), DMA((8,))],
        compiler_params=pltpu.CompilerParams(
            collective_id=1, has_side_effects=True, vmem_limit_bytes=6 * MIB
        ),
        name="exchange_back",
    )(src)


def factors_kernel(left, right, left_out, right_out, local, l_send, l_recv, send, recv):
    wide, narrow = lax.axis_index("wide"), lax.axis_index("narrow")
    seqs = right.shape[0]
    barrier = pltpu.get_barrier_semaphore()
    source_narrow = wide // 2
    for w in range(16):
        me = jnp.logical_and(wide == w, narrow == source_narrow)

        @pl.when(jnp.logical_not(me))
        def _():
            pl.semaphore_signal(
                barrier, inc=1, device_id=place(w, source_narrow), device_id_type=MESH
            )

    for peer in wide_peers():
        pl.semaphore_signal(barrier, inc=1, device_id=peer, device_id_type=MESH)
    selfish = (wide // 2) == narrow
    pl.semaphore_wait(barrier, 2 * 8 - selfish.astype(jnp.int32) + 4)

    own_right = pltpu.make_async_copy(right, right_out.at[pl.ds(wide * seqs, seqs)], local.at[0])
    own_right.start()

    def target(half, k):
        return 2 * narrow + half, narrow ^ k

    def left_copy(half, k):
        w, n = target(half, k)
        return remote(
            left.at[half], left_out.at[wide], l_send.at[half, k], l_recv.at[wide], place(w, n)
        )

    own_left = pltpu.make_async_copy(left.at[wide % 2], left_out.at[wide], local.at[1])

    def send_left():
        for k in (5, 4, 7, 6, 3, 2, 1, 0):
            for half in range(2):
                if k:
                    left_copy(half, k).start()
                else:
                    me = jnp.logical_and(selfish, wide % 2 == half)

                    @pl.when(jnp.logical_not(me))
                    def _():
                        left_copy(half, k).start()

                    @pl.when(me)
                    def _():
                        own_left.start()

    gather_wide(right_out, seqs, send, recv, source=right, then=send_left)
    own_right.wait()

    for w in range(16):
        me = jnp.logical_and(selfish, wide == w)

        @pl.when(jnp.logical_not(me))
        def _():
            slot = left_out.at[w]
            remote(
                slot, slot, l_send.at[0, 0], l_recv.at[w], place(w, source_narrow)
            ).wait_recv()

    @pl.when(selfish)
    def _():
        own_left.wait()

    for k in range(8):
        for half in range(2):
            if k:
                left_copy(half, k).wait_send()
            else:
                me = jnp.logical_and(selfish, wide % 2 == half)

                @pl.when(jnp.logical_not(me))
                def _():
                    left_copy(half, k).wait_send()


def exchange_factors(left, right, wide_size):
    return pl.pallas_call(
        factors_kernel,
        in_specs=[whole(), whole()],
        out_specs=[whole(pl.ANY), whole(pl.ANY)],
        out_shape=[
            jax.ShapeDtypeStruct((wide_size, *left.shape[1:]), F32),
            jax.ShapeDtypeStruct((wide_size * right.shape[0], *right.shape[1:]), F32),
        ],
        scratch_shapes=[DMA((2,)), DMA((2, 8)), DMA((16,)), DMA((19,)), DMA((19,))],
        compiler_params=pltpu.CompilerParams(
            collective_id=2, has_side_effects=True, vmem_limit_bytes=8 * MIB
        ),
        name="exchange_factors",
    )(left, right)


def attention_kernel(qkv_ref, bias_ref, out_ref, q_s, k_s, v_s, w_s):
    blocks, seqs, stacked, res = qkv_ref.shape
    width = stacked // 3

    @pl.when(pl.program_id(0) == 0)
    def _():
        pad = jnp.zeros((width, res), F32)
        for s in range(seqs):
            for b in range(blocks):
                cols = slice(b * res, (b + 1) * res)
                q_hi, q_lo = split32(qkv_ref[b, s, 0:width, :])
                k_hi, k_lo = split32(qkv_ref[b, s, width : 2 * width, :])
                v_hi, v_lo = split32(qkv_ref[b, s, 2 * width :, :])
                q_s[s, cols, :] = jnp.concatenate([q_hi, q_hi, q_lo, q_lo], axis=0).T.astype(BF16)
                k_s[s, :, cols] = jnp.concatenate([k_hi, k_lo, k_hi, k_lo], axis=0).astype(BF16)
                one = jnp.ones_like(pad)
                v_s[s, cols, :] = jnp.concatenate([v_hi, v_lo, one, pad], axis=0).T.astype(BF16)
                w_s[s, cols, :] = jnp.concatenate([v_hi, pad, one, pad], axis=0).T.astype(BF16)

    step = pl.program_id(0)
    rows = bias_ref.shape[0]
    start = pl.multiple_of(step * rows, rows)
    def sequence(s):
        scores = dot(q_s[s, pl.ds(start, rows), :], k_s[s]) + bias_ref[...]
        top = jnp.max(scores, axis=-1, keepdims=True)
        p_hi, p_lo = split(jnp.exp2(scores - top))
        mixed = (dot(p_hi, v_s[s]) + dot(p_lo, w_s[s])).T
        mixed = (mixed[:width] + mixed[width : 2 * width]) / mixed[2 * width : 3 * width]
        for b in range(rows // res):
            out_ref[b, s] = mixed[:, b * res : (b + 1) * res]

    for s in range(seqs):
        pl.when(step >= 0)(functools.partial(sequence, s))


def attention(qkv, bias):
    blocks, seqs, stacked, res = qkv.shape
    width = stacked // 3
    span = blocks * res
    return pl.pallas_call(
        attention_kernel,
        grid=(blocks // 4,),
        in_specs=[full(qkv.shape), pl.BlockSpec((4 * res, span), lambda i: (i, 0))],
        out_specs=pl.BlockSpec((4, seqs, width, res), lambda i: (i, 0, 0, 0)),
        out_shape=jax.ShapeDtypeStruct((blocks, seqs, width, res), F32),
        scratch_shapes=[
            pltpu.VMEM((seqs, span, 4 * width), BF16),
            pltpu.VMEM((seqs, 4 * width, span), BF16),
            pltpu.VMEM((seqs, span, 4 * width), BF16),
            pltpu.VMEM((seqs, span, 4 * width), BF16),
        ],
        compiler_params=pltpu.CompilerParams(vmem_limit_bytes=44 * MIB),
        name="attention",
    )(qkv, bias)


def mix_kernel(o_ref, gate_ref, x_ref, w_ref, off_ref, f_ref, s_ref, next_ref, left_ref, right_ref):
    heads, seqs, width, res = o_ref.shape
    channels = heads * width
    w_hi, w_lo = split(w_ref[...])
    pieces = []
    for s in range(seqs):
        stacked = o_ref[:, s].reshape(channels, res)
        pieces.append(stacked.T)
    attended = jnp.concatenate(pieces, axis=0) * gate_ref[...].reshape(seqs * res, channels)
    a_hi, a_lo = split(attended)
    x = x_ref[...].reshape(seqs * res, channels)
    after = x + dot3(a_hi, a_lo, w_hi, w_lo) + off_ref[...]
    next_ref[...] = after.reshape(seqs, res, channels)
    n_hi, n_lo = split(normalize(after))
    first = f_ref[...]
    f_hi, f_lo = split(jnp.concatenate([first] * 4 + [s_ref[...]] * 4, axis=0))
    y = dot_nt(n_hi, f_hi) + dot_nt(n_hi, f_lo) + dot_nt(n_lo, f_hi)
    hidden = first.shape[0]
    quarter = lax.broadcasted_iota(jnp.int32, (res // 8, 128), 1) // hidden
    for s in range(seqs):
        left = y[s * res : (s + 1) * res, :128]
        for half in range(2):
            rows = left[half * res // 2 : (half + 1) * res // 2].reshape(4, res // 8, 128)
            picked = rows[0]
            for q in range(1, 4):
                picked = jnp.where(quarter == q, rows[q], picked)
            left_ref[half, s] = picked
        right_ref[s] = y[s * res : (s + 1) * res, 128:].T[:hidden]


def mix(o, gate, x, w, offset, first, second):
    seqs, res, channels = x.shape
    hidden = first.shape[1]
    return pl.pallas_call(
        mix_kernel,
        in_specs=[whole()] * 7,
        out_specs=[whole()] * 3,
        out_shape=[
            jax.ShapeDtypeStruct(x.shape, F32),
            jax.ShapeDtypeStruct((2, seqs, res // 8, 128), F32),
            jax.ShapeDtypeStruct((seqs, hidden, res), F32),
        ],
        compiler_params=pltpu.CompilerParams(vmem_limit_bytes=16 * MIB),
        name="mix",
    )(o, gate, x, w, offset.reshape(1, channels), first.T, second.T)


def pair_kernel(
    left_ref, right_ref, pair_ref, w_ref, ob_ref, up_ref, eb_ref, down_ref, out_ref,
    l_s, r_s, wt_s, u_s, d_s, oh_s, ol_s, mid_s,
):
    cols, channels = pair_ref.shape[2:]
    seqs = r_s.shape[0] // 4
    groups = left_ref.shape[0] // seqs
    hidden = right_ref.shape[0] // seqs
    span = hidden * hidden

    @pl.when(pl.program_id(0) == 0)
    def _():
        def left_rows(r, carry):
            hi, lo = split32(left_ref[pl.ds(r, seqs, stride=groups), :])
            at = pl.ds(pl.multiple_of(r * 128, 128), 128)
            l_s[at, 0:128] = jnp.concatenate([hi, hi], axis=0).T.astype(BF16)
            l_s[at, 128:256] = jnp.concatenate([lo, lo], axis=0).T.astype(BF16)
            return carry

        lax.fori_loop(0, groups, left_rows, 0, unroll=4)

        def right_columns(d, carry):
            hi, lo = split(right_ref[pl.ds(d, seqs, stride=hidden), :])
            at = pl.ds(pl.multiple_of(d * cols, cols), cols)
            r_s[:, at] = jnp.concatenate([hi, lo, hi, lo], axis=0)
            return carry

        lax.fori_loop(0, hidden, right_columns, 0, unroll=4)

        def outer_weights(b, carry):
            rows = [w_ref[pl.ds(b * 4 + e, hidden, stride=hidden), :] for e in range(4)]
            w_hi, w_lo = split32(jnp.concatenate(rows, axis=0).T)
            at = pl.ds(pl.multiple_of(b * 128, 128), 128)
            wt_s[0:channels, at] = w_hi.astype(BF16)
            wt_s[channels : 2 * channels, at] = w_lo.astype(BF16)
            return carry

        lax.fori_loop(0, span // 128, outer_weights, 0, unroll=2)
        u_hi, u_lo = split(up_ref[...])
        u_s[0:channels] = u_hi
        u_s[channels : 2 * channels] = u_hi
        u_s[2 * channels :] = u_lo
        d_hi, d_lo = split(down_ref[...])
        d_s[:, 0:channels] = d_hi
        d_s[:, channels:] = d_lo

    step = pl.program_id(0)
    lhs = l_s[pl.ds(pl.multiple_of(step * 256, 256), 256), :]
    for d2 in range(hidden // 2):
        o_hi, o_lo = split(dot(lhs, r_s[:, d2 * 2 * cols : (d2 + 1) * 2 * cols]))
        for r2 in range(2):
            for q in range(4):
                rows = slice((r2 * 4 + q) * hidden, (r2 * 4 + q + 1) * hidden)
                for e in range(2):
                    d = d2 * 2 + e
                    at = (q, slice(d * hidden, (d + 1) * hidden), slice(r2 * cols, (r2 + 1) * cols))
                    oh_s[at] = o_hi[rows, e * cols : (e + 1) * cols]
                    ol_s[at] = o_lo[rows, e * cols : (e + 1) * cols]
    for q in range(4):
        first = dot(wt_s[...], oh_s[q])
        update = first[:channels] + first[channels:] + dot(wt_s[0:channels], ol_s[q])
        update = update.T * (1.0 / seqs)
        mid_s[q * 2 * cols : (q + 1) * 2 * cols, :] = (
            pair_ref[q].reshape(2 * cols, channels) + update + ob_ref[...]
        )

    def transition(part, carry):
        at = pl.ds(pl.multiple_of(part * 1024, 1024), 1024)
        mid = mid_s[at, :]
        n_hi, n_lo = split(normalize(mid))
        pre = dot(jnp.concatenate([n_hi, n_lo], axis=1), u_s[0 : 2 * channels])
        pre = pre + dot(n_hi, u_s[2 * channels :])
        h_hi, h_lo = split(jnp.maximum(pre + eb_ref[...], 0.0))
        wide = dot(h_hi, d_s[...])
        result = mid + wide[:, :channels] + wide[:, channels:] + dot(h_lo, d_s[:, 0:channels])
        mid_s[at, :] = result
        return carry

    pl.when(step >= 0)(lambda: transition(0, None) and None)

    for q in range(4):
        out_ref[q] = mid_s[q * 2 * cols : (q + 1) * 2 * cols, :].reshape(2, cols, channels)


def pair_update(left, right, pair_state, w, ob, up, eb, down):
    rows, cols, channels = pair_state.shape
    seqs, groups, lanes = left.shape
    hidden = right.shape[1]
    left = left.reshape(seqs * groups, lanes)
    right = right.reshape(seqs * hidden, cols)
    ft = up.shape[1]
    view = pair_state.reshape(4, rows // 4, cols, channels)
    block = pl.BlockSpec((4, 2, cols, channels), lambda i: (0, i, 0, 0))
    out = pl.pallas_call(
        pair_kernel,
        grid=(rows // 8,),
        in_specs=[
            full(left.shape),
            full(right.shape),
            block,
            full(w.shape),
            full((1, channels)),
            full(up.shape),
            full((1, ft)),
            full(down.shape),
        ],
        out_specs=block,
        out_shape=jax.ShapeDtypeStruct(view.shape, F32),
        scratch_shapes=[
            pltpu.VMEM((groups * lanes, 4 * seqs), BF16),
            pltpu.VMEM((4 * seqs, hidden * cols), BF16),
            pltpu.VMEM((2 * channels, hidden * hidden), BF16),
            pltpu.VMEM((3 * channels, ft), BF16),
            pltpu.VMEM((ft, 2 * channels), BF16),
            pltpu.VMEM((4, hidden * hidden, 2 * cols), BF16),
            pltpu.VMEM((4, hidden * hidden, 2 * cols), BF16),
            pltpu.VMEM((8 * cols, channels), F32),
        ],
        compiler_params=pltpu.CompilerParams(vmem_limit_bytes=48 * MIB),
        name="pair_update",
    )(left, right, view, w, ob.reshape(1, channels), up, eb.reshape(1, ft), down)
    return out.reshape(pair_state.shape)


def per_device(
    homolog_embedding,
    pair_state,
    probe_projector,
    lookup_projector,
    content_projector,
    sigmoid_projector,
    sigmoid_offset,
    pair_bias_weight,
    mixing_projector,
    mixing_offset,
    first_factor_projector,
    second_factor_projector,
    outer_product_weight,
    outer_product_bias,
    up_weight,
    expand_bias,
    down_weight,
):
    wide_size = lax.axis_size("wide")
    qkv_all, bias_all, gate = exchange_heads(
        homolog_embedding,
        probe_projector,
        lookup_projector,
        content_projector,
        sigmoid_projector,
        sigmoid_offset,
        pair_state,
        pair_bias_weight.T,
        wide_size,
    )
    mixed = attention(qkv_all, bias_all)
    back = exchange_back(mixed)
    after, left, right = mix(
        back,
        gate,
        homolog_embedding,
        mixing_projector,
        mixing_offset,
        first_factor_projector,
        second_factor_projector,
    )
    left_all, right_all = exchange_factors(left, right, wide_size)
    left_all = left_all.reshape(-1, *left_all.shape[2:])
    pair_next = pair_update(
        left_all,
        right_all,
        pair_state,
        outer_product_weight,
        outer_product_bias,
        up_weight,
        expand_bias,
        down_weight,
    )
    return after, pair_next


def solution(mesh):
    split_spec = P("wide", "narrow", None)
    return jax.shard_map(
        per_device,
        mesh=mesh,
        in_specs=(split_spec, split_spec) + (P(),) * 15,
        out_specs=(split_spec, split_spec),
        check_vma=False,
    )
```

```python
import functools
import math

import jax
import jax.numpy as jnp
from jax import lax
from jax.experimental import pallas as pl
from jax.experimental.pallas import tpu as pltpu
from jax.sharding import PartitionSpec as P

F32 = jnp.float32
BF16 = jnp.bfloat16
LOG2E = math.log2(math.e)
MIB = 1024 * 1024
MESH = pl.DeviceIdType.MESH

NT = (((1,), (1,)), ((), ()))


def dot(a, b):
    return jnp.dot(a, b, preferred_element_type=F32)


def dot_nt(a, b):
    return lax.dot_general(a, b, NT, preferred_element_type=F32)


def split(x):
    hi = x.astype(BF16)
    lo = (x - hi.astype(F32)).astype(BF16)
    return hi, lo


def split32(x):
    hi = x.astype(BF16).astype(F32)
    return hi, (x - hi).astype(BF16).astype(F32)


def dot3(a_hi, a_lo, b_hi, b_lo):
    return dot(a_hi, b_hi) + dot(a_hi, b_lo) + dot(a_lo, b_hi)


def normalize(x):
    mean = jnp.mean(x, axis=-1, keepdims=True)
    centered = x - mean
    variance = jnp.mean(centered * centered, axis=-1, keepdims=True)
    return centered * lax.rsqrt(variance + 1e-5)


def whole(memory_space=pltpu.VMEM):
    return pl.BlockSpec(memory_space=memory_space)


def full(shape):
    return pl.BlockSpec(shape, lambda *_: (0,) * len(shape))


def bias_rows(pair, w_t):
    rows, cols, channels = pair.shape
    heads = w_t.shape[0]
    n_hi, n_lo = split(normalize(pair.reshape(rows * cols, channels)))
    w_hi, w_lo = split32(w_t * LOG2E)
    top = jnp.concatenate([w_hi, w_hi], axis=1)
    low = jnp.concatenate([w_lo, jnp.zeros_like(w_lo)], axis=1)
    weights = jnp.concatenate([top, low], axis=0).astype(BF16)
    both = dot_nt(weights, jnp.concatenate([n_hi, n_lo], axis=1))
    return both[:heads] + both[heads:]


def place(wide, narrow):
    return {"wide": wide, "narrow": narrow}


def greet(peers):
    barrier = pltpu.get_barrier_semaphore()
    for peer in peers:
        pl.semaphore_signal(barrier, inc=1, device_id=peer, device_id_type=MESH)
    pl.semaphore_wait(barrier, len(peers))


def remote(src, dst, send, recv, peer):
    return pltpu.make_async_remote_copy(
        src_ref=src, dst_ref=dst, send_sem=send, recv_sem=recv, device_id=peer, device_id_type=MESH
    )


def wide_links(wide):
    z, x, core = wide // 4, (wide // 2) % 2, wide % 2
    at = lambda z_, x_, c_: (z_ * 2 + x_) * 2 + c_
    up, down, far = (z + 1) % 4, (z + 3) % 4, (z + 2) % 4
    return z, x, core, at, up, down, far


def gather_wide(buf, rows, send, recv, source=None, then=None):
    wide, narrow = lax.axis_index("wide"), lax.axis_index("narrow")
    z, x, core, at, up, down, far = wide_links(wide)
    other_x, other_core = 1 - x, 1 - core
    half = rows // 2

    def slab(z_, x_, c_, part=None):
        start = at(z_, x_, c_) * rows
        if part is None:
            return buf.at[pl.ds(start, rows)]
        return buf.at[pl.ds(start + part * half, half)]

    up_dev = place(at(up, x, core), narrow)
    down_dev = place(at(down, x, core), narrow)
    x_dev = place(at(z, other_x, core), narrow)
    core_dev = place(at(z, x, other_core), narrow)
    started = []
    count = [0]

    def push(region, index, dev):
        copy = remote(region, region, send.at[index], recv.at[index], dev)
        copy.start()
        started.append(copy)

    def arrived(region, index):
        remote(region, region, send.at[index], recv.at[index], core_dev).wait_recv()

    own = slab(z, x, core)
    for index, dev in ((0, x_dev), (1, up_dev), (2, down_dev), (9, core_dev)):
        copy = remote(own if source is None else source, own, send.at[index], recv.at[index], dev)
        copy.start()
        started.append(copy)
    if then is not None:
        then()
    expected = [(slab(z, x, other_core), 9)]

    def side(s, x_):
        below, above = slab(down, x_, core), slab(up, x_, core)
        base = 1 + 4 * s
        arrived(below, base)
        push(slab(down, x_, core, 0), base + 2, up_dev)
        push(below, 9 + base, core_dev)
        arrived(above, base + 1)
        push(slab(up, x_, core, 1), base + 3, down_dev)
        push(above, 9 + base + 1, core_dev)

    def finish(s, x_):
        base = 1 + 4 * s
        for part in range(2):
            region = slab(far, x_, core, part)
            arrived(region, base + 2 + part)
            push(region, 9 + base + 2 + part, core_dev)

    def partner(s, x_):
        base = 9 + 1 + 4 * s
        expected.append((slab(down, x_, other_core), base))
        expected.append((slab(up, x_, other_core), base + 1))
        for part in range(2):
            expected.append((slab(far, x_, other_core, part), base + 2 + part))

    cross = slab(z, other_x, core)
    arrived(cross, 0)
    push(cross, 5, up_dev)
    push(cross, 6, down_dev)
    push(cross, 18, core_dev)
    expected.append((slab(z, other_x, other_core), 18))
    side(0, x)
    finish(0, x)
    side(1, other_x)
    finish(1, other_x)
    partner(0, x)
    partner(1, other_x)
    for region, index in expected:
        arrived(region, index)
    for copy in started:
        copy.wait_send()


def wide_peers():
    wide, narrow = lax.axis_index("wide"), lax.axis_index("narrow")
    z, x, core, at, up, down, far = wide_links(wide)
    return [
        place(at(up, x, core), narrow),
        place(at(down, x, core), narrow),
        place(at(z, 1 - x, core), narrow),
        place(at(z, x, 1 - core), narrow),
    ]


def narrow_peers():
    wide, narrow = lax.axis_index("wide"), lax.axis_index("narrow")
    return [place(wide, narrow ^ k) for k in range(1, 8)]


BIAS_STEP = 32


def heads_kernel(
    x, wq, wk, wv, wg, offset, pair, weight, qkv_out, bias_out, gate_out,
    x_s, w_s, wb_s, tile, qkv, bias,
    load, load_w, local, b_send, b_recv, q_send, q_recv, send, recv,
):
    wide, narrow = lax.axis_index("wide"), lax.axis_index("narrow")
    rows, cols = bias.shape[1:]
    seqs, res, channels = x.shape
    heads = qkv.shape[0]
    width = channels // heads
    per_tile = 128 // width
    parts = rows // BIAS_STEP
    first_loads = [pltpu.make_async_copy(x, x_s, load_w.at[4])]
    for index, w in enumerate((wq, wk, wv, wg)):
        first_loads.append(pltpu.make_async_copy(w, w_s.at[index], load_w.at[index]))
    first_loads.append(pltpu.make_async_copy(weight, wb_s, load_w.at[5]))
    for copy in first_loads:
        copy.start()
    loads = []
    for part in range(parts):
        span = pl.ds(part * BIAS_STEP, BIAS_STEP)
        copy = pltpu.make_async_copy(pair.at[span], tile.at[span], load.at[part])
        copy.start()
        loads.append(copy)
    for copy in first_loads:
        copy.wait()

    n_hi, n_lo = split(normalize(x_s[...].reshape(seqs * res, channels)))
    scale = LOG2E / math.sqrt(width)
    for kind in range(3):
        y = dot3(n_hi, n_lo, *split(w_s[kind]))
        if kind == 0:
            y = y * scale
        for s in range(seqs):
            for t in range(channels // 128):
                turned = y[s * res : (s + 1) * res, t * 128 : (t + 1) * 128].T
                for h in range(per_tile):
                    qkv[t * per_tile + h, s, kind * width : (kind + 1) * width, :] = turned[
                        h * width : (h + 1) * width
                    ]
    greet(narrow_peers() + wide_peers())
    copies = []

    def send_qkv(ks):
        for k in ks:
            peer = narrow ^ k
            copy = remote(
                qkv.at[peer], qkv_out.at[narrow], q_send.at[k], q_recv.at[k], place(wide, peer)
            )
            copy.start()
            copies.append(copy)

    send_qkv((1, 2, 6))
    own_qkv = pltpu.make_async_copy(qkv.at[narrow], qkv_out.at[narrow], local.at[1])
    own_qkv.start()
    for part in range(parts):
        loads[part].wait()
        first = part * BIAS_STEP
        result = bias_rows(tile[first : first + BIAS_STEP], wb_s[...])
        for row in range(BIAS_STEP):
            bias[:, first + row, :] = result[:, row * cols : (row + 1) * cols]

    def bias_slot(source):
        return bias_out.at[pl.ds(wide * rows, rows), pl.ds(source * cols, cols)]

    own_bias = pltpu.make_async_copy(bias.at[narrow], bias_slot(narrow), local.at[0])
    own_bias.start()
    for k in (1, 3, 7, 5, 2, 6, 4):
        peer = narrow ^ k
        copy = remote(
            bias.at[peer], bias_slot(narrow), b_send.at[k], b_recv.at[k], place(wide, peer)
        )
        copy.start()
        copies.append(copy)
    own_bias.wait()
    for k in range(1, 8):
        slot = bias_slot(narrow ^ k)
        remote(slot, slot, b_send.at[k], b_recv.at[k], place(wide, narrow ^ k)).wait_recv()

    def rest():
        send_qkv((3, 7, 5, 4))
        gate = dot3(n_hi, n_lo, *split(w_s[3])) + offset[...]
        gate_out[...] = jax.nn.sigmoid(gate).reshape(seqs, res, channels)

    gather_wide(bias_out, rows, send, recv, then=rest)
    for k in range(1, 8):
        slot = qkv_out.at[narrow ^ k]
        remote(slot, slot, q_send.at[k], q_recv.at[k], place(wide, narrow ^ k)).wait_recv()
    own_qkv.wait()
    for copy in copies:
        copy.wait_send()


DMA = pltpu.SemaphoreType.DMA


def exchange_heads(x, wq, wk, wv, wg, offset, pair_state, weight_t, wide_size):
    rows, cols, _ = pair_state.shape
    heads, pair_channels = weight_t.shape
    seqs, res, channels = x.shape
    width = channels // heads
    qkv = (heads, seqs, 3 * width, res)
    return pl.pallas_call(
        heads_kernel,
        in_specs=[whole(pltpu.HBM)] * 5 + [whole(), whole(pltpu.HBM), whole(pltpu.HBM)],
        out_specs=[whole(pl.ANY), whole(pl.ANY), whole()],
        out_shape=[
            jax.ShapeDtypeStruct(qkv, F32),
            jax.ShapeDtypeStruct((wide_size * rows, heads * cols), F32),
            jax.ShapeDtypeStruct(x.shape, F32),
        ],
        scratch_shapes=[
            pltpu.VMEM(x.shape, F32),
            pltpu.VMEM((4, channels, channels), F32),
            pltpu.VMEM((heads, pair_channels), F32),
            pltpu.VMEM(pair_state.shape, F32),
            pltpu.VMEM(qkv, F32),
            pltpu.VMEM((heads, rows, cols), F32),
            DMA((rows // BIAS_STEP,)),
            DMA((6,)),
            DMA((2,)),
            DMA((8,)),
            DMA((8,)),
            DMA((8,)),
            DMA((8,)),
            DMA((19,)),
            DMA((19,)),
        ],
        compiler_params=pltpu.CompilerParams(
            collective_id=0, has_side_effects=True, vmem_limit_bytes=54 * MIB
        ),
        name="exchange_heads",
    )(x, wq, wk, wv, wg, offset.reshape(1, channels), pair_state, weight_t)


def factors_kernel(
    left, right, outer_w, up, down, left_out, right_out, wt_out, u_out, d_out,
    local, l_send, l_recv, send, recv,
):
    wide, narrow = lax.axis_index("wide"), lax.axis_index("narrow")
    seqs = right.shape[0]
    barrier = pltpu.get_barrier_semaphore()
    source_narrow = wide // 2
    for w in range(16):
        me = jnp.logical_and(wide == w, narrow == source_narrow)

        @pl.when(jnp.logical_not(me))
        def _():
            pl.semaphore_signal(
                barrier, inc=1, device_id=place(w, source_narrow), device_id_type=MESH
            )

    for peer in wide_peers():
        pl.semaphore_signal(barrier, inc=1, device_id=peer, device_id_type=MESH)
    selfish = (wide // 2) == narrow
    pl.semaphore_wait(barrier, 2 * 8 - selfish.astype(jnp.int32) + 4)

    own_right = pltpu.make_async_copy(right, right_out.at[pl.ds(wide * seqs, seqs)], local.at[0])
    own_right.start()

    def target(half, k):
        return 2 * narrow + half, narrow ^ k

    def left_copy(half, k):
        w, n = target(half, k)
        return remote(
            left.at[half], left_out.at[wide], l_send.at[half, k], l_recv.at[wide], place(w, n)
        )

    own_left = pltpu.make_async_copy(left.at[wide % 2], left_out.at[wide], local.at[1])

    def send_left():
        for k in (5, 4, 7, 6, 3, 2, 1, 0):
            for half in range(2):
                if k:
                    left_copy(half, k).start()
                else:
                    me = jnp.logical_and(selfish, wide % 2 == half)

                    @pl.when(jnp.logical_not(me))
                    def _():
                        left_copy(half, k).start()

                    @pl.when(me)
                    def _():
                        own_left.start()

    def weights():
        send_left()
        span, channels = outer_w.shape
        hidden = right.shape[1]
        for b in range(span // 128):
            rows = [outer_w[pl.ds(b * 4 + e, hidden, stride=hidden), :] for e in range(4)]
            w_hi, w_lo = split32(jnp.concatenate(rows, axis=0).T)
            wt_out[0:channels, b * 128 : (b + 1) * 128] = w_hi.astype(BF16)
            wt_out[channels : 2 * channels, b * 128 : (b + 1) * 128] = w_lo.astype(BF16)
        u_hi, u_lo = split(up[...])
        u_out[0:channels] = u_hi
        u_out[channels : 2 * channels] = u_hi
        u_out[2 * channels :] = u_lo
        d_hi, d_lo = split(down[...])
        d_out[:, 0:channels] = d_hi
        d_out[:, channels:] = d_lo

    gather_wide(right_out, seqs, send, recv, source=right, then=weights)
    own_right.wait()

    for w in range(16):
        me = jnp.logical_and(selfish, wide == w)

        @pl.when(jnp.logical_not(me))
        def _():
            slot = left_out.at[w]
            remote(
                slot, slot, l_send.at[0, 0], l_recv.at[w], place(w, source_narrow)
            ).wait_recv()

    @pl.when(selfish)
    def _():
        own_left.wait()

    for k in range(8):
        for half in range(2):
            if k:
                left_copy(half, k).wait_send()
            else:
                me = jnp.logical_and(selfish, wide % 2 == half)

                @pl.when(jnp.logical_not(me))
                def _():
                    left_copy(half, k).wait_send()


def exchange_factors(left, right, w, up, down, wide_size):
    span, channels = w.shape
    ft = up.shape[1]
    return pl.pallas_call(
        factors_kernel,
        in_specs=[whole()] * 5,
        out_specs=[whole(pl.ANY)] * 2 + [whole()] * 3,
        out_shape=[
            jax.ShapeDtypeStruct((wide_size, *left.shape[1:]), F32),
            jax.ShapeDtypeStruct((wide_size * right.shape[0], *right.shape[1:]), F32),
            jax.ShapeDtypeStruct((2 * channels, span), BF16),
            jax.ShapeDtypeStruct((3 * channels, ft), BF16),
            jax.ShapeDtypeStruct((ft, 2 * channels), BF16),
        ],
        scratch_shapes=[DMA((2,)), DMA((2, 8)), DMA((16,)), DMA((19,)), DMA((19,))],
        compiler_params=pltpu.CompilerParams(
            collective_id=2, has_side_effects=True, vmem_limit_bytes=16 * MIB
        ),
        name="exchange_factors",
    )(left, right, w, up, down)


ATTENTION_ROWS = 512


def attention_kernel(qkv_ref, bias_ref, back, q_s, k_s, v_s, w_s, o_s, local, send, recv):
    wide, narrow = lax.axis_index("wide"), lax.axis_index("narrow")
    blocks, seqs, stacked, res = qkv_ref.shape
    width = stacked // 3
    pad = jnp.zeros((width, res), F32)
    one = jnp.ones_like(pad)
    for s in range(seqs):
        for b in range(blocks):
            cols = slice(b * res, (b + 1) * res)
            q_hi, q_lo = split32(qkv_ref[b, s, 0:width, :])
            k_hi, k_lo = split32(qkv_ref[b, s, width : 2 * width, :])
            v_hi, v_lo = split32(qkv_ref[b, s, 2 * width :, :])
            q_s[s, cols, :] = jnp.concatenate([q_hi, q_hi, q_lo, q_lo], axis=0).T.astype(BF16)
            k_s[s, :, cols] = jnp.concatenate([k_hi, k_lo, k_hi, k_lo], axis=0).astype(BF16)
            v_s[s, cols, :] = jnp.concatenate([v_hi, v_lo, one, pad], axis=0).T.astype(BF16)
            w_s[s, cols, :] = jnp.concatenate([v_hi, pad, one, pad], axis=0).T.astype(BF16)
    greet(narrow_peers())
    rows = ATTENTION_ROWS
    group = rows // res

    def piece(n, s):
        return remote(
            o_s.at[n, s], back.at[narrow, s], send.at[n, s], recv.at[narrow, s], place(wide, n)
        )

    def each(step, act):
        for b in range(group):
            n = step * group + b
            pl.when(n != narrow)(functools.partial(act, n))

    def rows_of(step, carry):
        start = pl.multiple_of(step * rows, rows)

        def sequence(s):
            scores = dot(q_s[s, pl.ds(start, rows), :], k_s[s]) + bias_ref[pl.ds(start, rows), :]
            top = jnp.max(scores, axis=-1, keepdims=True)
            p_hi, p_lo = split(jnp.exp2(scores - top))
            mixed = (dot(p_hi, v_s[s]) + dot(p_lo, w_s[s])).T
            mixed = (mixed[:width] + mixed[width : 2 * width]) / mixed[2 * width : 3 * width]
            for b in range(group):
                o_s[step * group + b, s] = mixed[:, b * res : (b + 1) * res]

        for s in range(seqs):
            pl.when(step >= 0)(functools.partial(sequence, s))
            if s:
                each(step, lambda n, s=s: piece(n, s - 1).start())
        each(step, lambda n: piece(n, 0).wait_send())
        each(step, lambda n: piece(n, seqs - 1).start())
        return carry

    lax.fori_loop(0, blocks // group, rows_of, 0)
    own = pltpu.make_async_copy(o_s.at[narrow], back.at[narrow], local)
    own.start()
    for k in range(1, 8):
        peer = narrow ^ k
        for s in range(1, seqs):
            piece(peer, s).wait_send()
    for k in range(1, 8):
        peer = narrow ^ k
        for s in range(seqs):
            slot = back.at[peer, s]
            remote(slot, slot, send.at[peer, s], recv.at[peer, s], place(wide, peer)).wait_recv()
    own.wait()


def attention(qkv, bias):
    blocks, seqs, stacked, res = qkv.shape
    width = stacked // 3
    span = blocks * res
    return pl.pallas_call(
        attention_kernel,
        in_specs=[whole(), whole()],
        out_specs=whole(pl.ANY),
        out_shape=jax.ShapeDtypeStruct((blocks, seqs, width, res), F32),
        scratch_shapes=[
            pltpu.VMEM((seqs, span, 4 * width), BF16),
            pltpu.VMEM((seqs, 4 * width, span), BF16),
            pltpu.VMEM((seqs, span, 4 * width), BF16),
            pltpu.VMEM((seqs, span, 4 * width), BF16),
            pltpu.VMEM((blocks, seqs, width, res), F32),
            DMA,
            DMA((blocks, seqs)),
            DMA((blocks, seqs)),
        ],
        compiler_params=pltpu.CompilerParams(
            collective_id=1, has_side_effects=True, vmem_limit_bytes=56 * MIB
        ),
        name="attention",
    )(qkv, bias)


def mix_kernel(o_ref, gate_ref, x_ref, w_ref, off_ref, f_ref, s_ref, next_ref, left_ref, right_ref):
    heads, seqs, width, res = o_ref.shape
    channels = heads * width
    w_hi, w_lo = split(w_ref[...])
    pieces = []
    for s in range(seqs):
        stacked = o_ref[:, s].reshape(channels, res)
        pieces.append(stacked.T)
    attended = jnp.concatenate(pieces, axis=0) * gate_ref[...].reshape(seqs * res, channels)
    a_hi, a_lo = split(attended)
    x = x_ref[...].reshape(seqs * res, channels)
    after = x + dot3(a_hi, a_lo, w_hi, w_lo) + off_ref[...]
    next_ref[...] = after.reshape(seqs, res, channels)
    n_hi, n_lo = split(normalize(after))
    first = f_ref[...]
    f_hi, f_lo = split(jnp.concatenate([first] * 4 + [s_ref[...]] * 4, axis=0))
    y = dot_nt(n_hi, f_hi) + dot_nt(n_hi, f_lo) + dot_nt(n_lo, f_hi)
    hidden = first.shape[0]
    quarter = lax.broadcasted_iota(jnp.int32, (res // 8, 128), 1) // hidden
    for s in range(seqs):
        left = y[s * res : (s + 1) * res, :128]
        for half in range(2):
            rows = left[half * res // 2 : (half + 1) * res // 2].reshape(4, res // 8, 128)
            picked = rows[0]
            for q in range(1, 4):
                picked = jnp.where(quarter == q, rows[q], picked)
            left_ref[half, s] = picked
        right_ref[s] = y[s * res : (s + 1) * res, 128:].T[:hidden]


def mix(o, gate, x, w, offset, first, second):
    seqs, res, channels = x.shape
    hidden = first.shape[1]
    return pl.pallas_call(
        mix_kernel,
        in_specs=[whole()] * 7,
        out_specs=[whole()] * 3,
        out_shape=[
            jax.ShapeDtypeStruct(x.shape, F32),
            jax.ShapeDtypeStruct((2, seqs, res // 8, 128), F32),
            jax.ShapeDtypeStruct((seqs, hidden, res), F32),
        ],
        compiler_params=pltpu.CompilerParams(vmem_limit_bytes=16 * MIB),
        name="mix",
    )(o, gate, x, w, offset.reshape(1, channels), first.T, second.T)


def pair_kernel(
    left_ref, right_ref, pair_ref, wt_s, ob_ref, u_s, eb_ref, d_s, out_ref,
    l_s, r_s, oh_s, ol_s, mid_s,
):
    cols, channels = pair_ref.shape[2:]
    seqs = r_s.shape[0] // 4
    groups = left_ref.shape[0] // seqs
    hidden = right_ref.shape[0] // seqs

    @pl.when(pl.program_id(0) == 0)
    def _():
        def left_rows(r, carry):
            hi, lo = split32(left_ref[pl.ds(r, seqs, stride=groups), :])
            at = pl.ds(pl.multiple_of(r * 128, 128), 128)
            l_s[at, 0:128] = jnp.concatenate([hi, hi], axis=0).T.astype(BF16)
            l_s[at, 128:256] = jnp.concatenate([lo, lo], axis=0).T.astype(BF16)
            return carry

        lax.fori_loop(0, groups, left_rows, 0, unroll=4)

        def right_columns(d, carry):
            hi, lo = split(right_ref[pl.ds(d, seqs, stride=hidden), :])
            at = pl.ds(pl.multiple_of(d * cols, cols), cols)
            r_s[:, at] = jnp.concatenate([hi, lo, hi, lo], axis=0)
            return carry

        lax.fori_loop(0, hidden, right_columns, 0, unroll=4)

    step = pl.program_id(0)
    lhs = l_s[pl.ds(pl.multiple_of(step * 256, 256), 256), :]
    for d2 in range(hidden // 2):
        o_hi, o_lo = split(dot(lhs, r_s[:, d2 * 2 * cols : (d2 + 1) * 2 * cols]))
        for r2 in range(2):
            for q in range(4):
                rows = slice((r2 * 4 + q) * hidden, (r2 * 4 + q + 1) * hidden)
                for e in range(2):
                    d = d2 * 2 + e
                    at = (q, slice(d * hidden, (d + 1) * hidden), slice(r2 * cols, (r2 + 1) * cols))
                    oh_s[at] = o_hi[rows, e * cols : (e + 1) * cols]
                    ol_s[at] = o_lo[rows, e * cols : (e + 1) * cols]
    for q in range(4):
        first = dot(wt_s[...], oh_s[q])
        update = first[:channels] + first[channels:] + dot(wt_s[0:channels], ol_s[q])
        update = update.T * (1.0 / seqs)
        mid_s[q * 2 * cols : (q + 1) * 2 * cols, :] = (
            pair_ref[q].reshape(2 * cols, channels) + update + ob_ref[...]
        )

    def transition(part, carry):
        at = pl.ds(pl.multiple_of(part * 1024, 1024), 1024)
        mid = mid_s[at, :]
        n_hi, n_lo = split(normalize(mid))
        pre = dot(jnp.concatenate([n_hi, n_lo], axis=1), u_s[0 : 2 * channels])
        pre = pre + dot(n_hi, u_s[2 * channels :])
        h_hi, h_lo = split(jnp.maximum(pre + eb_ref[...], 0.0))
        wide = dot(h_hi, d_s[...])
        result = mid + wide[:, :channels] + wide[:, channels:] + dot(h_lo, d_s[:, 0:channels])
        mid_s[at, :] = result
        return carry

    pl.when(step >= 0)(lambda: transition(0, None) and None)

    for q in range(4):
        out_ref[q] = mid_s[q * 2 * cols : (q + 1) * 2 * cols, :].reshape(2, cols, channels)


def pair_update(left, right, pair_state, wt, ob, up, eb, down):
    rows, cols, channels = pair_state.shape
    seqs, groups, lanes = left.shape
    hidden = right.shape[1]
    left = left.reshape(seqs * groups, lanes)
    right = right.reshape(seqs * hidden, cols)
    ft = up.shape[1]
    view = pair_state.reshape(4, rows // 4, cols, channels)
    block = pl.BlockSpec((4, 2, cols, channels), lambda i: (0, i, 0, 0))
    out = pl.pallas_call(
        pair_kernel,
        grid=(rows // 8,),
        in_specs=[
            full(left.shape),
            full(right.shape),
            block,
            full(wt.shape),
            full((1, channels)),
            full(up.shape),
            full((1, ft)),
            full(down.shape),
        ],
        out_specs=block,
        out_shape=jax.ShapeDtypeStruct(view.shape, F32),
        scratch_shapes=[
            pltpu.VMEM((groups * lanes, 4 * seqs), BF16),
            pltpu.VMEM((4 * seqs, hidden * cols), BF16),
            pltpu.VMEM((4, hidden * hidden, 2 * cols), BF16),
            pltpu.VMEM((4, hidden * hidden, 2 * cols), BF16),
            pltpu.VMEM((8 * cols, channels), F32),
        ],
        compiler_params=pltpu.CompilerParams(vmem_limit_bytes=48 * MIB),
        name="pair_update",
    )(left, right, view, wt, ob.reshape(1, channels), up, eb.reshape(1, ft), down)
    return out.reshape(pair_state.shape)


def per_device(
    homolog_embedding,
    pair_state,
    probe_projector,
    lookup_projector,
    content_projector,
    sigmoid_projector,
    sigmoid_offset,
    pair_bias_weight,
    mixing_projector,
    mixing_offset,
    first_factor_projector,
    second_factor_projector,
    outer_product_weight,
    outer_product_bias,
    up_weight,
    expand_bias,
    down_weight,
):
    wide_size = lax.axis_size("wide")
    qkv_all, bias_all, gate = exchange_heads(
        homolog_embedding,
        probe_projector,
        lookup_projector,
        content_projector,
        sigmoid_projector,
        sigmoid_offset,
        pair_state,
        pair_bias_weight.T,
        wide_size,
    )
    back = attention(qkv_all, bias_all)
    after, left, right = mix(
        back,
        gate,
        homolog_embedding,
        mixing_projector,
        mixing_offset,
        first_factor_projector,
        second_factor_projector,
    )
    left_all, right_all, wt, up, down = exchange_factors(
        left, right, outer_product_weight, up_weight, down_weight, wide_size
    )
    left_all = left_all.reshape(-1, *left_all.shape[2:])
    pair_next = pair_update(
        left_all,
        right_all,
        pair_state,
        wt,
        outer_product_bias,
        up,
        expand_bias,
        down,
    )
    return after, pair_next


def solution(mesh):
    split_spec = P("wide", "narrow", None)
    return jax.shard_map(
        per_device,
        mesh=mesh,
        in_specs=(split_spec, split_spec) + (P(),) * 15,
        out_specs=(split_spec, split_spec),
        check_vma=False,
    )
```

```python
import functools
import math

import jax
import jax.numpy as jnp
from jax import lax
from jax.experimental import pallas as pl
from jax.experimental.pallas import tpu as pltpu
from jax.sharding import PartitionSpec as P

F32 = jnp.float32
BF16 = jnp.bfloat16
LOG2E = math.log2(math.e)
MIB = 1024 * 1024
MESH = pl.DeviceIdType.MESH

NT = (((1,), (1,)), ((), ()))


def dot(a, b):
    return jnp.dot(a, b, preferred_element_type=F32)


def dot_nt(a, b):
    return lax.dot_general(a, b, NT, preferred_element_type=F32)


def split(x):
    hi = x.astype(BF16)
    lo = (x - hi.astype(F32)).astype(BF16)
    return hi, lo


def split32(x):
    hi = x.astype(BF16).astype(F32)
    return hi, (x - hi).astype(BF16).astype(F32)


def dot3(a_hi, a_lo, b_hi, b_lo):
    return dot(a_hi, b_hi) + dot(a_hi, b_lo) + dot(a_lo, b_hi)


def normalize(x):
    mean = jnp.mean(x, axis=-1, keepdims=True)
    centered = x - mean
    variance = jnp.mean(centered * centered, axis=-1, keepdims=True)
    return centered * lax.rsqrt(variance + 1e-5)


def whole(memory_space=pltpu.VMEM):
    return pl.BlockSpec(memory_space=memory_space)


def full(shape):
    return pl.BlockSpec(shape, lambda *_: (0,) * len(shape))


def bias_rows(pair, w_t):
    rows, cols, channels = pair.shape
    heads = w_t.shape[0]
    n_hi, n_lo = split(normalize(pair.reshape(rows * cols, channels)))
    w_hi, w_lo = split32(w_t * LOG2E)
    top = jnp.concatenate([w_hi, w_hi], axis=1)
    low = jnp.concatenate([w_lo, jnp.zeros_like(w_lo)], axis=1)
    weights = jnp.concatenate([top, low], axis=0).astype(BF16)
    both = dot_nt(weights, jnp.concatenate([n_hi, n_lo], axis=1))
    return both[:heads] + both[heads:]


def place(wide, narrow):
    return {"wide": wide, "narrow": narrow}


def announce(peers):
    barrier = pltpu.get_barrier_semaphore()
    for peer in peers:
        pl.semaphore_signal(barrier, inc=1, device_id=peer, device_id_type=MESH)


def await_peers(peers):
    pl.semaphore_wait(pltpu.get_barrier_semaphore(), len(peers))


def remote(src, dst, send, recv, peer):
    return pltpu.make_async_remote_copy(
        src_ref=src, dst_ref=dst, send_sem=send, recv_sem=recv, device_id=peer, device_id_type=MESH
    )


def wide_links(wide):
    z, x, core = wide // 4, (wide // 2) % 2, wide % 2
    at = lambda z_, x_, c_: (z_ * 2 + x_) * 2 + c_
    up, down, far = (z + 1) % 4, (z + 3) % 4, (z + 2) % 4
    return z, x, core, at, up, down, far


def gather_wide(buf, rows, send, recv, source=None, then=None):
    wide, narrow = lax.axis_index("wide"), lax.axis_index("narrow")
    z, x, core, at, up, down, far = wide_links(wide)
    other_x, other_core = 1 - x, 1 - core
    half = rows // 2

    def slab(z_, x_, c_, part=None):
        start = at(z_, x_, c_) * rows
        if part is None:
            return buf.at[pl.ds(start, rows)]
        return buf.at[pl.ds(start + part * half, half)]

    up_dev = place(at(up, x, core), narrow)
    down_dev = place(at(down, x, core), narrow)
    x_dev = place(at(z, other_x, core), narrow)
    core_dev = place(at(z, x, other_core), narrow)
    started = []
    count = [0]

    def push(region, index, dev):
        copy = remote(region, region, send.at[index], recv.at[index], dev)
        copy.start()
        started.append(copy)

    def arrived(region, index):
        remote(region, region, send.at[index], recv.at[index], core_dev).wait_recv()

    own = slab(z, x, core)
    for index, dev in ((0, x_dev), (1, up_dev), (2, down_dev), (9, core_dev)):
        copy = remote(own if source is None else source, own, send.at[index], recv.at[index], dev)
        copy.start()
        started.append(copy)
    if then is not None:
        then()
    expected = [(slab(z, x, other_core), 9)]

    def side(s, x_):
        below, above = slab(down, x_, core), slab(up, x_, core)
        base = 1 + 4 * s
        arrived(below, base)
        push(slab(down, x_, core, 0), base + 2, up_dev)
        push(below, 9 + base, core_dev)
        arrived(above, base + 1)
        push(slab(up, x_, core, 1), base + 3, down_dev)
        push(above, 9 + base + 1, core_dev)

    def finish(s, x_):
        base = 1 + 4 * s
        for part in range(2):
            region = slab(far, x_, core, part)
            arrived(region, base + 2 + part)
            push(region, 9 + base + 2 + part, core_dev)

    def partner(s, x_):
        base = 9 + 1 + 4 * s
        expected.append((slab(down, x_, other_core), base))
        expected.append((slab(up, x_, other_core), base + 1))
        for part in range(2):
            expected.append((slab(far, x_, other_core, part), base + 2 + part))

    cross = slab(z, other_x, core)
    arrived(cross, 0)
    push(cross, 5, up_dev)
    push(cross, 6, down_dev)
    push(cross, 18, core_dev)
    expected.append((slab(z, other_x, other_core), 18))
    side(0, x)
    finish(0, x)
    side(1, other_x)
    finish(1, other_x)
    partner(0, x)
    partner(1, other_x)
    for region, index in expected:
        arrived(region, index)
    for copy in started:
        copy.wait_send()


def wide_peers():
    wide, narrow = lax.axis_index("wide"), lax.axis_index("narrow")
    z, x, core, at, up, down, far = wide_links(wide)
    return [
        place(at(up, x, core), narrow),
        place(at(down, x, core), narrow),
        place(at(z, 1 - x, core), narrow),
        place(at(z, x, 1 - core), narrow),
    ]


def narrow_peers():
    wide, narrow = lax.axis_index("wide"), lax.axis_index("narrow")
    return [place(wide, narrow ^ k) for k in range(1, 8)]


BIAS_STEP = 32


def heads_kernel(
    x, wq, wk, wv, wg, offset, pair, weight, qkv_out, bias_out, gate_out,
    x_s, w_s, wb_s, tile, qkv, bias,
    load, load_w, local, b_send, b_recv, q_send, q_recv, send, recv,
):
    wide, narrow = lax.axis_index("wide"), lax.axis_index("narrow")
    rows, cols = bias.shape[1:]
    seqs, res, channels = x.shape
    heads = qkv.shape[0]
    width = channels // heads
    per_tile = 128 // width
    parts = rows // BIAS_STEP
    peers = narrow_peers() + wide_peers()
    announce(peers)
    first_loads = [pltpu.make_async_copy(x, x_s, load_w.at[4])]
    for index, w in enumerate((wq, wk, wv, wg)):
        first_loads.append(pltpu.make_async_copy(w, w_s.at[index], load_w.at[index]))
    first_loads.append(pltpu.make_async_copy(weight, wb_s, load_w.at[5]))
    for copy in first_loads:
        copy.start()
    loads = []
    for part in range(parts):
        span = pl.ds(part * BIAS_STEP, BIAS_STEP)
        copy = pltpu.make_async_copy(pair.at[span], tile.at[span], load.at[part])
        copy.start()
        loads.append(copy)
    for copy in first_loads:
        copy.wait()

    n_hi, n_lo = split(normalize(x_s[...].reshape(seqs * res, channels)))
    scale = LOG2E / math.sqrt(width)
    for kind in range(3):
        y = dot3(n_hi, n_lo, *split(w_s[kind]))
        if kind == 0:
            y = y * scale
        for s in range(seqs):
            for t in range(channels // 128):
                turned = y[s * res : (s + 1) * res, t * 128 : (t + 1) * 128].T
                for h in range(per_tile):
                    qkv[t * per_tile + h, s, kind * width : (kind + 1) * width, :] = turned[
                        h * width : (h + 1) * width
                    ]
    await_peers(peers)
    copies = []

    def send_qkv(ks):
        for k in ks:
            peer = narrow ^ k
            copy = remote(
                qkv.at[peer], qkv_out.at[narrow], q_send.at[k], q_recv.at[k], place(wide, peer)
            )
            copy.start()
            copies.append(copy)

    send_qkv((1, 2, 6))
    own_qkv = pltpu.make_async_copy(qkv.at[narrow], qkv_out.at[narrow], local.at[1])
    own_qkv.start()
    for part in range(parts):
        loads[part].wait()
        first = part * BIAS_STEP
        result = bias_rows(tile[first : first + BIAS_STEP], wb_s[...])
        for row in range(BIAS_STEP):
            bias[:, first + row, :] = result[:, row * cols : (row + 1) * cols]

    def bias_slot(source):
        return bias_out.at[pl.ds(wide * rows, rows), pl.ds(source * cols, cols)]

    own_bias = pltpu.make_async_copy(bias.at[narrow], bias_slot(narrow), local.at[0])
    own_bias.start()
    for k in (1, 3, 7, 5, 2, 6, 4):
        peer = narrow ^ k
        copy = remote(
            bias.at[peer], bias_slot(narrow), b_send.at[k], b_recv.at[k], place(wide, peer)
        )
        copy.start()
        copies.append(copy)
    own_bias.wait()
    for k in range(1, 8):
        slot = bias_slot(narrow ^ k)
        remote(slot, slot, b_send.at[k], b_recv.at[k], place(wide, narrow ^ k)).wait_recv()

    def rest():
        send_qkv((3, 7, 5, 4))
        gate = dot3(n_hi, n_lo, *split(w_s[3])) + offset[...]
        gate_out[...] = jax.nn.sigmoid(gate).reshape(seqs, res, channels)

    gather_wide(bias_out, rows, send, recv, then=rest)
    for k in range(1, 8):
        slot = qkv_out.at[narrow ^ k]
        remote(slot, slot, q_send.at[k], q_recv.at[k], place(wide, narrow ^ k)).wait_recv()
    own_qkv.wait()
    for copy in copies:
        copy.wait_send()


DMA = pltpu.SemaphoreType.DMA


def exchange_heads(x, wq, wk, wv, wg, offset, pair_state, weight_t, wide_size):
    rows, cols, _ = pair_state.shape
    heads, pair_channels = weight_t.shape
    seqs, res, channels = x.shape
    width = channels // heads
    qkv = (heads, seqs, 3 * width, res)
    return pl.pallas_call(
        heads_kernel,
        in_specs=[whole(pltpu.HBM)] * 5 + [whole(), whole(pltpu.HBM), whole(pltpu.HBM)],
        out_specs=[whole(pl.ANY), whole(pl.ANY), whole()],
        out_shape=[
            jax.ShapeDtypeStruct(qkv, F32),
            jax.ShapeDtypeStruct((wide_size * rows, heads * cols), F32),
            jax.ShapeDtypeStruct(x.shape, F32),
        ],
        scratch_shapes=[
            pltpu.VMEM(x.shape, F32),
            pltpu.VMEM((4, channels, channels), F32),
            pltpu.VMEM((heads, pair_channels), F32),
            pltpu.VMEM(pair_state.shape, F32),
            pltpu.VMEM(qkv, F32),
            pltpu.VMEM((heads, rows, cols), F32),
            DMA((rows // BIAS_STEP,)),
            DMA((6,)),
            DMA((2,)),
            DMA((8,)),
            DMA((8,)),
            DMA((8,)),
            DMA((8,)),
            DMA((19,)),
            DMA((19,)),
        ],
        compiler_params=pltpu.CompilerParams(
            collective_id=0, has_side_effects=True, vmem_limit_bytes=54 * MIB
        ),
        name="exchange_heads",
    )(x, wq, wk, wv, wg, offset.reshape(1, channels), pair_state, weight_t)


def factors_kernel(
    left, right, outer_w, up, down, left_out, right_out, wt_out, u_out, d_out,
    local, l_send, l_recv, send, recv,
):
    wide, narrow = lax.axis_index("wide"), lax.axis_index("narrow")
    seqs = right.shape[0]
    barrier = pltpu.get_barrier_semaphore()
    source_narrow = wide // 2
    for w in range(16):
        me = jnp.logical_and(wide == w, narrow == source_narrow)

        @pl.when(jnp.logical_not(me))
        def _():
            pl.semaphore_signal(
                barrier, inc=1, device_id=place(w, source_narrow), device_id_type=MESH
            )

    for peer in wide_peers():
        pl.semaphore_signal(barrier, inc=1, device_id=peer, device_id_type=MESH)
    selfish = (wide // 2) == narrow
    pl.semaphore_wait(barrier, 2 * 8 - selfish.astype(jnp.int32) + 4)

    own_right = pltpu.make_async_copy(right, right_out.at[pl.ds(wide * seqs, seqs)], local.at[0])
    own_right.start()

    def target(half, k):
        return 2 * narrow + half, narrow ^ k

    def left_copy(half, k):
        w, n = target(half, k)
        return remote(
            left.at[half], left_out.at[wide], l_send.at[half, k], l_recv.at[wide], place(w, n)
        )

    own_left = pltpu.make_async_copy(left.at[wide % 2], left_out.at[wide], local.at[1])

    def send_left():
        for k in (5, 4, 7, 6, 3, 2, 1, 0):
            for half in range(2):
                if k:
                    left_copy(half, k).start()
                else:
                    me = jnp.logical_and(selfish, wide % 2 == half)

                    @pl.when(jnp.logical_not(me))
                    def _():
                        left_copy(half, k).start()

                    @pl.when(me)
                    def _():
                        own_left.start()

    def weights():
        send_left()
        span, channels = outer_w.shape
        hidden = right.shape[1]
        for b in range(span // 128):
            rows = [outer_w[pl.ds(b * 4 + e, hidden, stride=hidden), :] for e in range(4)]
            w_hi, w_lo = split32(jnp.concatenate(rows, axis=0).T)
            wt_out[0:channels, b * 128 : (b + 1) * 128] = w_hi.astype(BF16)
            wt_out[channels : 2 * channels, b * 128 : (b + 1) * 128] = w_lo.astype(BF16)
        u_hi, u_lo = split(up[...])
        u_out[0:channels] = u_hi
        u_out[channels : 2 * channels] = u_hi
        u_out[2 * channels :] = u_lo
        d_hi, d_lo = split(down[...])
        d_out[:, 0:channels] = d_hi
        d_out[:, channels:] = d_lo

    gather_wide(right_out, seqs, send, recv, source=right, then=weights)
    own_right.wait()

    for w in range(16):
        me = jnp.logical_and(selfish, wide == w)

        @pl.when(jnp.logical_not(me))
        def _():
            slot = left_out.at[w]
            remote(
                slot, slot, l_send.at[0, 0], l_recv.at[w], place(w, source_narrow)
            ).wait_recv()

    @pl.when(selfish)
    def _():
        own_left.wait()

    for k in range(8):
        for half in range(2):
            if k:
                left_copy(half, k).wait_send()
            else:
                me = jnp.logical_and(selfish, wide % 2 == half)

                @pl.when(jnp.logical_not(me))
                def _():
                    left_copy(half, k).wait_send()


def exchange_factors(left, right, w, up, down, wide_size):
    span, channels = w.shape
    ft = up.shape[1]
    return pl.pallas_call(
        factors_kernel,
        in_specs=[whole()] * 5,
        out_specs=[whole(pl.ANY)] * 2 + [whole()] * 3,
        out_shape=[
            jax.ShapeDtypeStruct((wide_size, *left.shape[1:]), F32),
            jax.ShapeDtypeStruct((wide_size * right.shape[0], *right.shape[1:]), F32),
            jax.ShapeDtypeStruct((2 * channels, span), BF16),
            jax.ShapeDtypeStruct((3 * channels, ft), BF16),
            jax.ShapeDtypeStruct((ft, 2 * channels), BF16),
        ],
        scratch_shapes=[DMA((2,)), DMA((2, 8)), DMA((16,)), DMA((19,)), DMA((19,))],
        compiler_params=pltpu.CompilerParams(
            collective_id=2, has_side_effects=True, vmem_limit_bytes=16 * MIB
        ),
        name="exchange_factors",
    )(left, right, w, up, down)


ATTENTION_ROWS = 512


def attention_kernel(qkv_ref, bias_ref, back, q_s, k_s, v_s, w_s, o_s, local, send, recv):
    wide, narrow = lax.axis_index("wide"), lax.axis_index("narrow")
    blocks, seqs, stacked, res = qkv_ref.shape
    width = stacked // 3
    peers = narrow_peers()
    announce(peers)
    pad = jnp.zeros((width, res), F32)
    one = jnp.ones_like(pad)
    for s in range(seqs):
        for b in range(blocks):
            cols = slice(b * res, (b + 1) * res)
            q_hi, q_lo = split32(qkv_ref[b, s, 0:width, :])
            k_hi, k_lo = split32(qkv_ref[b, s, width : 2 * width, :])
            v_hi, v_lo = split32(qkv_ref[b, s, 2 * width :, :])
            q_s[s, cols, :] = jnp.concatenate([q_hi, q_hi, q_lo, q_lo], axis=0).T.astype(BF16)
            k_s[s, :, cols] = jnp.concatenate([k_hi, k_lo, k_hi, k_lo], axis=0).astype(BF16)
            v_s[s, cols, :] = jnp.concatenate([v_hi, v_lo, one, pad], axis=0).T.astype(BF16)
            w_s[s, cols, :] = jnp.concatenate([v_hi, pad, one, pad], axis=0).T.astype(BF16)
    await_peers(peers)
    rows = ATTENTION_ROWS
    group = rows // res

    def piece(n, s):
        return remote(
            o_s.at[n, s], back.at[narrow, s], send.at[n, s], recv.at[narrow, s], place(wide, n)
        )

    def each(step, act):
        for b in range(group):
            n = step * group + b
            pl.when(n != narrow)(functools.partial(act, n))

    def rows_of(step, carry):
        start = pl.multiple_of(step * rows, rows)

        def sequence(s):
            scores = dot(q_s[s, pl.ds(start, rows), :], k_s[s]) + bias_ref[pl.ds(start, rows), :]
            top = jnp.max(scores, axis=-1, keepdims=True)
            p_hi, p_lo = split(jnp.exp2(scores - top))
            mixed = (dot(p_hi, v_s[s]) + dot(p_lo, w_s[s])).T
            mixed = (mixed[:width] + mixed[width : 2 * width]) / mixed[2 * width : 3 * width]
            for b in range(group):
                o_s[step * group + b, s] = mixed[:, b * res : (b + 1) * res]

        for s in range(seqs):
            pl.when(step >= 0)(functools.partial(sequence, s))
            if s:
                each(step, lambda n, s=s: piece(n, s - 1).start())
        each(step, lambda n: piece(n, 0).wait_send())
        each(step, lambda n: piece(n, seqs - 1).start())
        return carry

    lax.fori_loop(0, blocks // group, rows_of, 0)
    own = pltpu.make_async_copy(o_s.at[narrow], back.at[narrow], local)
    own.start()
    for k in range(1, 8):
        peer = narrow ^ k
        for s in range(1, seqs):
            piece(peer, s).wait_send()
    for k in range(1, 8):
        peer = narrow ^ k
        for s in range(seqs):
            slot = back.at[peer, s]
            remote(slot, slot, send.at[peer, s], recv.at[peer, s], place(wide, peer)).wait_recv()
    own.wait()


def attention(qkv, bias):
    blocks, seqs, stacked, res = qkv.shape
    width = stacked // 3
    span = blocks * res
    return pl.pallas_call(
        attention_kernel,
        in_specs=[whole(), whole()],
        out_specs=whole(pl.ANY),
        out_shape=jax.ShapeDtypeStruct((blocks, seqs, width, res), F32),
        scratch_shapes=[
            pltpu.VMEM((seqs, span, 4 * width), BF16),
            pltpu.VMEM((seqs, 4 * width, span), BF16),
            pltpu.VMEM((seqs, span, 4 * width), BF16),
            pltpu.VMEM((seqs, span, 4 * width), BF16),
            pltpu.VMEM((blocks, seqs, width, res), F32),
            DMA,
            DMA((blocks, seqs)),
            DMA((blocks, seqs)),
        ],
        compiler_params=pltpu.CompilerParams(
            collective_id=1, has_side_effects=True, vmem_limit_bytes=56 * MIB
        ),
        name="attention",
    )(qkv, bias)


def mix_kernel(o_ref, gate_ref, x_ref, w_ref, off_ref, f_ref, s_ref, next_ref, left_ref, right_ref):
    heads, seqs, width, res = o_ref.shape
    channels = heads * width
    w_hi, w_lo = split(w_ref[...])
    pieces = []
    for s in range(seqs):
        stacked = o_ref[:, s].reshape(channels, res)
        pieces.append(stacked.T)
    attended = jnp.concatenate(pieces, axis=0) * gate_ref[...].reshape(seqs * res, channels)
    a_hi, a_lo = split(attended)
    x = x_ref[...].reshape(seqs * res, channels)
    after = x + dot3(a_hi, a_lo, w_hi, w_lo) + off_ref[...]
    next_ref[...] = after.reshape(seqs, res, channels)
    n_hi, n_lo = split(normalize(after))
    first = f_ref[...]
    f_hi, f_lo = split(jnp.concatenate([first] * 4 + [s_ref[...]] * 4, axis=0))
    y = dot_nt(n_hi, f_hi) + dot_nt(n_hi, f_lo) + dot_nt(n_lo, f_hi)
    hidden = first.shape[0]
    quarter = lax.broadcasted_iota(jnp.int32, (res // 8, 128), 1) // hidden
    for s in range(seqs):
        left = y[s * res : (s + 1) * res, :128]
        for half in range(2):
            rows = left[half * res // 2 : (half + 1) * res // 2].reshape(4, res // 8, 128)
            picked = rows[0]
            for q in range(1, 4):
                picked = jnp.where(quarter == q, rows[q], picked)
            left_ref[half, s] = picked
        right_ref[s] = y[s * res : (s + 1) * res, 128:].T[:hidden]


def mix(o, gate, x, w, offset, first, second):
    seqs, res, channels = x.shape
    hidden = first.shape[1]
    return pl.pallas_call(
        mix_kernel,
        in_specs=[whole()] * 7,
        out_specs=[whole()] * 3,
        out_shape=[
            jax.ShapeDtypeStruct(x.shape, F32),
            jax.ShapeDtypeStruct((2, seqs, res // 8, 128), F32),
            jax.ShapeDtypeStruct((seqs, hidden, res), F32),
        ],
        compiler_params=pltpu.CompilerParams(vmem_limit_bytes=16 * MIB),
        name="mix",
    )(o, gate, x, w, offset.reshape(1, channels), first.T, second.T)


def pair_kernel(
    left_ref, right_ref, pair_ref, wt_s, ob_ref, u_s, eb_ref, d_s, out_ref,
    l_s, r_s, oh_s, ol_s, mid_s,
):
    cols, channels = pair_ref.shape[2:]
    seqs = r_s.shape[0] // 4
    groups = left_ref.shape[0] // seqs
    hidden = right_ref.shape[0] // seqs

    @pl.when(pl.program_id(0) == 0)
    def _():
        def left_rows(r, carry):
            hi, lo = split32(left_ref[pl.ds(r, seqs, stride=groups), :])
            at = pl.ds(pl.multiple_of(r * 128, 128), 128)
            l_s[at, 0:128] = jnp.concatenate([hi, hi], axis=0).T.astype(BF16)
            l_s[at, 128:256] = jnp.concatenate([lo, lo], axis=0).T.astype(BF16)
            return carry

        lax.fori_loop(0, groups, left_rows, 0, unroll=4)

        def right_columns(d, carry):
            hi, lo = split(right_ref[pl.ds(d, seqs, stride=hidden), :])
            at = pl.ds(pl.multiple_of(d * cols, cols), cols)
            r_s[:, at] = jnp.concatenate([hi, lo, hi, lo], axis=0)
            return carry

        lax.fori_loop(0, hidden, right_columns, 0, unroll=4)

    step = pl.program_id(0)
    lhs = l_s[pl.ds(pl.multiple_of(step * 256, 256), 256), :]
    for d2 in range(hidden // 2):
        o_hi, o_lo = split(dot(lhs, r_s[:, d2 * 2 * cols : (d2 + 1) * 2 * cols]))
        for r2 in range(2):
            for q in range(4):
                rows = slice((r2 * 4 + q) * hidden, (r2 * 4 + q + 1) * hidden)
                for e in range(2):
                    d = d2 * 2 + e
                    at = (q, slice(d * hidden, (d + 1) * hidden), slice(r2 * cols, (r2 + 1) * cols))
                    oh_s[at] = o_hi[rows, e * cols : (e + 1) * cols]
                    ol_s[at] = o_lo[rows, e * cols : (e + 1) * cols]
    for q in range(4):
        first = dot(wt_s[...], oh_s[q])
        update = first[:channels] + first[channels:] + dot(wt_s[0:channels], ol_s[q])
        update = update.T * (1.0 / seqs)
        mid_s[q * 2 * cols : (q + 1) * 2 * cols, :] = (
            pair_ref[q].reshape(2 * cols, channels) + update + ob_ref[...]
        )

    def transition(part, carry):
        at = pl.ds(pl.multiple_of(part * 1024, 1024), 1024)
        mid = mid_s[at, :]
        n_hi, n_lo = split(normalize(mid))
        pre = dot(jnp.concatenate([n_hi, n_lo], axis=1), u_s[0 : 2 * channels])
        pre = pre + dot(n_hi, u_s[2 * channels :])
        h_hi, h_lo = split(jnp.maximum(pre + eb_ref[...], 0.0))
        wide = dot(h_hi, d_s[...])
        result = mid + wide[:, :channels] + wide[:, channels:] + dot(h_lo, d_s[:, 0:channels])
        mid_s[at, :] = result
        return carry

    pl.when(step >= 0)(lambda: transition(0, None) and None)

    for q in range(4):
        out_ref[q] = mid_s[q * 2 * cols : (q + 1) * 2 * cols, :].reshape(2, cols, channels)


def pair_update(left, right, pair_state, wt, ob, up, eb, down):
    rows, cols, channels = pair_state.shape
    seqs, groups, lanes = left.shape
    hidden = right.shape[1]
    left = left.reshape(seqs * groups, lanes)
    right = right.reshape(seqs * hidden, cols)
    ft = up.shape[1]
    view = pair_state.reshape(4, rows // 4, cols, channels)
    block = pl.BlockSpec((4, 2, cols, channels), lambda i: (0, i, 0, 0))
    out = pl.pallas_call(
        pair_kernel,
        grid=(rows // 8,),
        in_specs=[
            full(left.shape),
            full(right.shape),
            block,
            full(wt.shape),
            full((1, channels)),
            full(up.shape),
            full((1, ft)),
            full(down.shape),
        ],
        out_specs=block,
        out_shape=jax.ShapeDtypeStruct(view.shape, F32),
        scratch_shapes=[
            pltpu.VMEM((groups * lanes, 4 * seqs), BF16),
            pltpu.VMEM((4 * seqs, hidden * cols), BF16),
            pltpu.VMEM((4, hidden * hidden, 2 * cols), BF16),
            pltpu.VMEM((4, hidden * hidden, 2 * cols), BF16),
            pltpu.VMEM((8 * cols, channels), F32),
        ],
        compiler_params=pltpu.CompilerParams(vmem_limit_bytes=48 * MIB),
        name="pair_update",
    )(left, right, view, wt, ob.reshape(1, channels), up, eb.reshape(1, ft), down)
    return out.reshape(pair_state.shape)


def per_device(
    homolog_embedding,
    pair_state,
    probe_projector,
    lookup_projector,
    content_projector,
    sigmoid_projector,
    sigmoid_offset,
    pair_bias_weight,
    mixing_projector,
    mixing_offset,
    first_factor_projector,
    second_factor_projector,
    outer_product_weight,
    outer_product_bias,
    up_weight,
    expand_bias,
    down_weight,
):
    wide_size = lax.axis_size("wide")
    qkv_all, bias_all, gate = exchange_heads(
        homolog_embedding,
        probe_projector,
        lookup_projector,
        content_projector,
        sigmoid_projector,
        sigmoid_offset,
        pair_state,
        pair_bias_weight.T,
        wide_size,
    )
    back = attention(qkv_all, bias_all)
    after, left, right = mix(
        back,
        gate,
        homolog_embedding,
        mixing_projector,
        mixing_offset,
        first_factor_projector,
        second_factor_projector,
    )
    left_all, right_all, wt, up, down = exchange_factors(
        left, right, outer_product_weight, up_weight, down_weight, wide_size
    )
    left_all = left_all.reshape(-1, *left_all.shape[2:])
    pair_next = pair_update(
        left_all,
        right_all,
        pair_state,
        wt,
        outer_product_bias,
        up,
        expand_bias,
        down,
    )
    return after, pair_next


def solution(mesh):
    split_spec = P("wide", "narrow", None)
    return jax.shard_map(
        per_device,
        mesh=mesh,
        in_specs=(split_spec, split_spec) + (P(),) * 15,
        out_specs=(split_spec, split_spec),
        check_vma=False,
    )
```
